32 devices in a mesh: dp: 2 (over x), tx: 4 (over z), tyz: 4 (over y, core).
Axes of the slice: x: 2, y: 2, z: 4, core: 2. Of those that a mesh axis runs over, the one named last changes fastest.
Arguments:
- residual: bfloat16 [2048, 2560], P('dp', ('tx', 'tyz')), parts along dimension 0
- ln_scale: bfloat16 [2560], P(('tx', 'tyz'))
- w_query: bfloat16 [2560, 2560], P('tx', 'tyz')
- w_key: bfloat16 [2560, 80], P('tx')
- w_value: bfloat16 [2560, 80], P('tx')
- w_gate: bfloat16 [2560, 10240], P('tx', 'tyz')
- w_up: bfloat16 [2560, 10240], P('tx', 'tyz')
- w_out: bfloat16 [2560, 2560], P('tyz', 'tx')
- w_down: bfloat16 [10240, 2560], P('tyz', 'tx')
- k_cache: bfloat16 [2048, 1024, 80], P(('dp', 'tx', 'tyz')), parts along dimension 0
- v_cache: bfloat16 [2048, 1024, 80], P(('dp', 'tx', 'tyz')), parts along dimension 0
- lengths: int32 [2048], P(('dp', 'tx', 'tyz')), parts along dimension 0
Outputs:
- output 1: bfloat16 [2048, 2560], P('dp', ('tx', 'tyz')), parts along dimension 0
- output 2: bfloat16 [2048, 1024, 80], P(('dp', 'tx', 'tyz')), parts along dimension 0
- output 3: bfloat16 [2048, 1024, 80], P(('dp', 'tx', 'tyz')), parts along dimension 0
There are 2 independent parts. The reference program is written for one: setup_inputs(seed, part) draws one part's arguments, and reference() takes and returns one part's arrays. A program takes and returns all parts, laid end to end along the dimension named above; an argument that names none is the same for every part.
All inputs are finite; a program needn't handle non-finite values.
Results may differ from the reference program's by a relative error of at most 0.0155287.
Values are sent between devices in bfloat16 or wider.
A program may use at most 1 GiB of HBM per device.

```python
import jax
import jax.numpy as jnp
from jax import lax

MODEL_DIM = 2560
FF_DIM = 10240
NUM_HEADS = 32
HEAD_DIM = 80
SEQ_LEN = 1024
BATCH_ROWS = 1024
ROW_BLOCK = 64
LN_EPS = 1e-5
ROPE_BASE = 10000.0


def draw_lengths(len_key):
    low_key, pick_key = jax.random.split(len_key)
    drawn_lens = jax.random.randint(low_key, (BATCH_ROWS,), SEQ_LEN // 8, SEQ_LEN, dtype=jnp.int32)
    row_order = jax.random.permutation(pick_key, BATCH_ROWS)
    row_ids = jnp.arange(BATCH_ROWS)
    drawn_lens = jnp.where(row_ids == row_order[0], SEQ_LEN - 1, drawn_lens)
    drawn_lens = jnp.where(row_ids == row_order[1], SEQ_LEN // 8, drawn_lens)
    return drawn_lens.astype(jnp.int32)


def setup_inputs(seed: int = 0, part: int = 0) -> dict:
    part_keys = jax.random.split(jax.random.fold_in(jax.random.key(seed), part), 4)
    shared_keys = jax.random.split(jax.random.key(seed + 1), 8)
    q_width = NUM_HEADS * HEAD_DIM
    in_scale = MODEL_DIM ** -0.5
    out_scale = 0.3 * (SEQ_LEN / q_width) ** 0.5
    down_scale = FF_DIM ** -0.5
    return {
        'residual': jax.random.normal(part_keys[0], (BATCH_ROWS, MODEL_DIM), jnp.float32).astype(jnp.bfloat16),
        'ln_scale': (1.0 + 0.4 * jax.random.normal(shared_keys[0], (MODEL_DIM,), jnp.float32)).astype(jnp.bfloat16),
        'w_query': (jax.random.normal(shared_keys[1], (MODEL_DIM, q_width), jnp.float32) * in_scale).astype(jnp.bfloat16),
        'w_key': (jax.random.normal(shared_keys[2], (MODEL_DIM, HEAD_DIM), jnp.float32) * in_scale).astype(jnp.bfloat16),
        'w_value': (jax.random.normal(shared_keys[3], (MODEL_DIM, HEAD_DIM), jnp.float32) * in_scale).astype(jnp.bfloat16),
        'w_gate': (jax.random.normal(shared_keys[4], (MODEL_DIM, FF_DIM), jnp.float32) * in_scale).astype(jnp.bfloat16),
        'w_up': (jax.random.normal(shared_keys[5], (MODEL_DIM, FF_DIM), jnp.float32) * in_scale).astype(jnp.bfloat16),
        'w_out': (jax.random.normal(shared_keys[6], (q_width, MODEL_DIM), jnp.float32) * out_scale).astype(jnp.bfloat16),
        'w_down': (jax.random.normal(shared_keys[7], (FF_DIM, MODEL_DIM), jnp.float32) * down_scale).astype(jnp.bfloat16),
        'k_cache': jax.random.normal(part_keys[1], (BATCH_ROWS, SEQ_LEN, HEAD_DIM), jnp.float32).astype(jnp.bfloat16),
        'v_cache': jax.random.normal(part_keys[2], (BATCH_ROWS, SEQ_LEN, HEAD_DIM), jnp.float32).astype(jnp.bfloat16),
        'lengths': draw_lengths(part_keys[3]),
    }


def rope_rotate(vectors, positions):
    head_dim = vectors.shape[-1]
    half_dim = head_dim // 2
    inv_freq = ROPE_BASE ** (-2.0 * jnp.arange(half_dim, dtype=jnp.float32) / head_dim)
    angles = positions.astype(jnp.float32)[:, None] * inv_freq[None, :]
    bcast_shape = (angles.shape[0],) + (1,) * (vectors.ndim - 2) + (half_dim,)
    cos_part = jnp.cos(angles).reshape(bcast_shape)
    sin_part = jnp.sin(angles).reshape(bcast_shape)
    vec_f32 = vectors.astype(jnp.float32)
    first_half = vec_f32[..., :half_dim]
    second_half = vec_f32[..., half_dim:]
    rotated = jnp.concatenate([first_half * cos_part - second_half * sin_part, second_half * cos_part + first_half * sin_part], axis=-1)
    return rotated.astype(jnp.bfloat16)


def attend_rows(query_rot, key_rot, value_new, k_cache, v_cache, lengths):
    positions = jnp.arange(k_cache.shape[1], dtype=jnp.int32)
    write_mask = (positions[None, :] == lengths[:, None])[:, :, None]
    k_updated = jnp.where(write_mask, key_rot[:, None, :], k_cache)
    v_updated = jnp.where(write_mask, value_new[:, None, :], v_cache)
    scores = jnp.einsum('rhd,rtd->rht', query_rot.astype(jnp.float32), k_updated.astype(jnp.float32)) * (query_rot.shape[-1] ** -0.5)
    valid_mask = (positions[None, :] <= lengths[:, None])[:, None, :]
    scores = jnp.where(valid_mask, scores, -1e30)
    attn_probs = jax.nn.softmax(scores, axis=-1).astype(jnp.bfloat16)
    attended = jnp.einsum('rht,rtd->rhd', attn_probs.astype(jnp.float32), v_updated.astype(jnp.float32)).astype(jnp.bfloat16)
    return attended, k_updated, v_updated


def reference(residual, ln_scale, w_query, w_key, w_value, w_gate, w_up, w_out, w_down, k_cache, v_cache, lengths):
    res_f32 = residual.astype(jnp.float32)
    row_mean = jnp.mean(res_f32, axis=-1, keepdims=True)
    row_var = jnp.mean(jnp.square(res_f32 - row_mean), axis=-1, keepdims=True)
    normed = ((res_f32 - row_mean) * lax.rsqrt(row_var + LN_EPS) * ln_scale.astype(jnp.float32)).astype(jnp.bfloat16)
    query_vec = jnp.dot(normed, w_query, preferred_element_type=jnp.float32).astype(jnp.bfloat16)
    key_new = jnp.dot(normed, w_key, preferred_element_type=jnp.float32).astype(jnp.bfloat16)
    value_new = jnp.dot(normed, w_value, preferred_element_type=jnp.float32).astype(jnp.bfloat16)
    gate_val = jnp.dot(normed, w_gate, preferred_element_type=jnp.float32).astype(jnp.bfloat16)
    up_val = jnp.dot(normed, w_up, preferred_element_type=jnp.float32).astype(jnp.bfloat16)
    mlp_act = (jax.nn.silu(gate_val.astype(jnp.float32)) * up_val.astype(jnp.float32)).astype(jnp.bfloat16)
    query_rot = rope_rotate(query_vec.reshape(BATCH_ROWS, NUM_HEADS, HEAD_DIM), lengths)
    key_rot = rope_rotate(key_new, lengths)
    num_blocks = BATCH_ROWS // ROW_BLOCK

    def attend_block(block_args):
        return attend_rows(block_args[0], block_args[1], block_args[2], block_args[3], block_args[4], block_args[5])

    attended, k_blocks, v_blocks = lax.map(attend_block, (
        query_rot.reshape(num_blocks, ROW_BLOCK, NUM_HEADS, HEAD_DIM),
        key_rot.reshape(num_blocks, ROW_BLOCK, HEAD_DIM),
        value_new.reshape(num_blocks, ROW_BLOCK, HEAD_DIM),
        k_cache.reshape(num_blocks, ROW_BLOCK, SEQ_LEN, HEAD_DIM),
        v_cache.reshape(num_blocks, ROW_BLOCK, SEQ_LEN, HEAD_DIM),
        lengths.reshape(num_blocks, ROW_BLOCK)))
    attn_flat = attended.reshape(BATCH_ROWS, NUM_HEADS * HEAD_DIM)
    block_out = jnp.dot(attn_flat, w_out, preferred_element_type=jnp.float32) + jnp.dot(mlp_act, w_down, preferred_element_type=jnp.float32)
    new_resid = (res_f32 + block_out).astype(jnp.bfloat16)
    return (new_resid, k_blocks.reshape(BATCH_ROWS, SEQ_LEN, HEAD_DIM), v_blocks.reshape(BATCH_ROWS, SEQ_LEN, HEAD_DIM))
```

```python
import functools

import jax
import jax.numpy as jnp
from jax import lax
from jax.experimental import pallas as pl
from jax.experimental.pallas import tpu as pltpu
from jax.sharding import PartitionSpec as P

LN_EPS = 1e-5
ROPE_BASE = 10000.0
MESH = pl.DeviceIdType.MESH
NZ = 4
EXTRA = 16


def position():
    dp = lax.axis_index("dp")
    z = lax.axis_index("tx")
    ty = lax.axis_index("tyz")
    return dp, z, ty // 2, ty % 2


def neighbour_barrier(dp, z, y, c):
    sem = pltpu.get_barrier_semaphore()

    def greet(device):
        pl.semaphore_signal(sem, inc=1, device_id=device, device_id_type=MESH)

    pl.when(z > 0)(lambda: greet((dp, z - 1, y * 2 + c)))
    pl.when(z < NZ - 1)(lambda: greet((dp, z + 1, y * 2 + c)))
    greet((dp, z, (1 - y) * 2 + c))
    greet((dp, z, y * 2 + 1 - c))
    inner = jnp.logical_and(z > 0, z < NZ - 1)
    pl.when(inner)(lambda: pl.semaphore_wait(sem, 4))
    pl.when(jnp.logical_not(inner))(lambda: pl.semaphore_wait(sem, 3))


def gather_kernel(x_ref, out_ref, lsem, zs, zr, ys, yr, cs, cr):
    dp, z, y, c = position()
    ty = y * 2 + c
    peer_y, peer_c = (1 - y) * 2 + c, y * 2 + 1 - c
    local = pltpu.make_async_copy(x_ref, out_ref.at[0, ty], lsem)
    local.start()
    neighbour_barrier(dp, z, y, c)
    local.wait()

    def z_copy(o, step):
        slot = lax.rem(o + step + NZ, NZ)
        return pltpu.make_async_remote_copy(
            out_ref.at[o, ty], out_ref.at[slot, ty],
            zs.at[o, (step + 1) // 2], zr.at[slot], device_id=(dp, z + step, ty), device_id_type=MESH)

    def z_arrived(o):
        return pltpu.make_async_remote_copy(
            out_ref.at[o, ty], out_ref.at[o, ty], zs.at[o, 0], zr.at[o],
            device_id=(dp, z, peer_y), device_id_type=MESH)

    def y_copy(o):
        return pltpu.make_async_remote_copy(
            out_ref.at[o, ty], out_ref.at[o, ty], ys.at[o], yr.at[o],
            device_id=(dp, z, peer_y), device_id_type=MESH)

    def y_arrived(o):
        return pltpu.make_async_remote_copy(
            out_ref.at[o, peer_y], out_ref.at[o, peer_y], ys.at[o], yr.at[o],
            device_id=(dp, z, peer_y), device_id_type=MESH)

    def c_copy(o, yy):
        return pltpu.make_async_remote_copy(
            out_ref.at[o, yy * 2 + c], out_ref.at[o, yy * 2 + c], cs.at[o, yy], cr.at[o, yy],
            device_id=(dp, z, peer_c), device_id_type=MESH)

    def c_arrived(o, yy):
        return pltpu.make_async_remote_copy(
            out_ref.at[o, yy * 2 + 1 - c], out_ref.at[o, yy * 2 + 1 - c], cs.at[o, yy], cr.at[o, yy],
            device_id=(dp, z, peer_c), device_id_type=MESH)

    pl.when(z < NZ - 1)(lambda: z_copy(0, 1).start())
    pl.when(z > 0)(lambda: z_copy(0, -1).start())
    y_copy(0).start()
    c_copy(0, y).start()
    for d in range(1, NZ):
        for o, here, onward, step in (
                (d, z >= d, z < NZ - 1, 1), (NZ - d, z + d < NZ, z > 0, -1)):
            def handle(o=o, onward=onward, step=step):
                z_arrived(o).wait_recv()
                pl.when(onward)(lambda: z_copy(o, step).start())
                y_copy(o).start()
                c_copy(o, y).start()
            pl.when(here)(handle)
    for d in range(NZ):
        for o, here in ((d, z >= d), (NZ - d, z + d < NZ)):
            if d == 0 and o == NZ:
                continue

            def handle(o=o):
                y_arrived(o).wait_recv()
                c_copy(o, 1 - y).start()
            pl.when(here)(handle)
    for o in range(NZ):
        y_copy(o).wait_send()
        for yy in range(2):
            c_copy(o, yy).wait_send()
            c_arrived(o, yy).wait_recv()
    pl.when(z < NZ - 1)(lambda: z_copy(0, 1).wait_send())
    pl.when(z > 0)(lambda: z_copy(0, -1).wait_send())
    for d in range(1, NZ):
        pl.when(jnp.logical_and(z >= d, z < NZ - 1))(lambda d=d: z_copy(d, 1).wait_send())
        pl.when(jnp.logical_and(z + d < NZ, z > 0))(lambda d=d: z_copy(NZ - d, -1).wait_send())


def gather_blocks(block):
    rows, lanes = block.shape
    dma = pltpu.SemaphoreType.DMA
    return pl.pallas_call(
        gather_kernel,
        out_shape=jax.ShapeDtypeStruct((NZ, 4, rows, lanes), block.dtype),
        in_specs=[pl.BlockSpec(memory_space=pl.ANY)],
        out_specs=pl.BlockSpec(memory_space=pltpu.VMEM),
        scratch_shapes=[dma, dma((NZ, 2)), dma((NZ,)), dma((NZ,)), dma((NZ,)), dma((NZ, 2)), dma((NZ, 2))],
        compiler_params=pltpu.CompilerParams(collective_id=0, has_side_effects=True,
                                             vmem_limit_bytes=12 * 2**20),
        name="gather_blocks",
    )(block)


def reduce_kernel(p_ref, res_ref, out_ref, cbuf, ysend, yrecv, zsend, zrecv, cs, cr, ys, yr, zs, zr):
    dp, z, y, c = position()
    ty = y * 2 + c
    peer_y, peer_c = (1 - y) * 2 + c, y * 2 + 1 - c
    neighbour_barrier(dp, z, y, c)

    def c_copy(o, yy):
        return pltpu.make_async_remote_copy(
            p_ref.at[o, yy * 2 + 1 - c], cbuf.at[o, yy], cs.at[o, yy], cr.at[o, yy],
            device_id=(dp, z, peer_c), device_id_type=MESH)

    def y_copy(o):
        return pltpu.make_async_remote_copy(
            ysend.at[o], yrecv.at[o], ys.at[o], yr.at[o],
            device_id=(dp, z, peer_y), device_id_type=MESH)

    def z_copy(o, step):
        slot = lax.rem(o + step + NZ, NZ)
        side = (1 - step) // 2
        return pltpu.make_async_remote_copy(
            zsend.at[o], zrecv.at[side, slot], zs.at[o], zr.at[side, slot],
            device_id=(dp, z + step, ty), device_id_type=MESH)

    def z_arrived(o, side):
        return pltpu.make_async_remote_copy(
            zsend.at[o], zrecv.at[side, o], zs.at[o], zr.at[side, o],
            device_id=(dp, z, peer_y), device_id_type=MESH)

    order = []
    for d in range(NZ - 1, 0, -1):
        order += [(NZ - d, z + d < NZ, 1), (d, z >= d, -1)]

    for yy in (1 - y, y):
        for o, here, _ in order:
            pl.when(here)(lambda o=o, yy=yy: c_copy(o, yy).start())
        c_copy(0, yy).start()

    def to_y(o):
        c_copy(o, 1 - y).wait_recv()
        ysend[o] = (p_ref[o, peer_y].astype(jnp.float32)
                    + cbuf[o, 1 - y].astype(jnp.float32)).astype(jnp.bfloat16)
        y_copy(o).start()

    for o, here, _ in order:
        pl.when(here)(functools.partial(to_y, o))
    to_y(0)

    def chip_pair_sum(o):
        c_copy(o, y).wait_recv()
        y_copy(o).wait_recv()
        return (p_ref[o, ty].astype(jnp.float32) + cbuf[o, y].astype(jnp.float32)
                + yrecv[o].astype(jnp.float32))

    def to_z(o, step):
        total = chip_pair_sum(o)
        side = (1 - step) // 2
        more = z > 0 if step == 1 else z < NZ - 1

        @pl.when(more)
        def _():
            z_arrived(o, side).wait_recv()
            zsend[o] = (total + zrecv[side, o].astype(jnp.float32)).astype(jnp.bfloat16)

        @pl.when(jnp.logical_not(more))
        def _():
            zsend[o] = total.astype(jnp.bfloat16)
        z_copy(o, step).start()

    for o, here, step in order:
        pl.when(here)(functools.partial(to_z, o, step))

    total = chip_pair_sum(0) + res_ref[...].astype(jnp.float32)

    @pl.when(z == 0)
    def _():
        z_arrived(0, 1).wait_recv()
        out_ref[...] = (total + zrecv[1, 0].astype(jnp.float32)).astype(jnp.bfloat16)

    @pl.when(z == NZ - 1)
    def _():
        z_arrived(0, 0).wait_recv()
        out_ref[...] = (total + zrecv[0, 0].astype(jnp.float32)).astype(jnp.bfloat16)

    @pl.when(jnp.logical_and(z > 0, z < NZ - 1))
    def _():
        z_arrived(0, 0).wait_recv()
        z_arrived(0, 1).wait_recv()
        out_ref[...] = (total + zrecv[0, 0].astype(jnp.float32)
                        + zrecv[1, 0].astype(jnp.float32)).astype(jnp.bfloat16)

    for o in range(NZ):
        y_copy(o).wait_send()
        for yy in range(2):
            c_copy(o, yy).wait_send()
    for o, here, step in order:
        pl.when(here)(lambda o=o, step=step: z_copy(o, step).wait_send())


def reduce_blocks(parts, residual):
    _, _, rows, lanes = parts.shape
    dma = pltpu.SemaphoreType.DMA
    vmem = pl.BlockSpec(memory_space=pltpu.VMEM)
    buf = lambda *lead: pltpu.VMEM(lead + (rows, lanes), jnp.bfloat16)
    return pl.pallas_call(
        reduce_kernel,
        out_shape=jax.ShapeDtypeStruct((rows, lanes), jnp.bfloat16),
        in_specs=[vmem, vmem], out_specs=vmem,
        scratch_shapes=[buf(NZ, 2), buf(NZ), buf(NZ), buf(NZ), buf(2, NZ),
                        dma((NZ, 2)), dma((NZ, 2)), dma((NZ,)), dma((NZ,)), dma((NZ,)), dma((2, NZ))],
        compiler_params=pltpu.CompilerParams(collective_id=1, has_side_effects=True,
                                             vmem_limit_bytes=24 * 2**20),
        name="reduce_blocks",
    )(parts, residual)


def rope_rotate(vectors, positions):
    head_dim = vectors.shape[-1]
    half_dim = head_dim // 2
    inv_freq = ROPE_BASE ** (-2.0 * jnp.arange(half_dim, dtype=jnp.float32) / head_dim)
    angles = positions.astype(jnp.float32)[:, None] * inv_freq[None, :]
    bcast_shape = (angles.shape[0],) + (1,) * (vectors.ndim - 2) + (half_dim,)
    cos_part = jnp.cos(angles).reshape(bcast_shape)
    sin_part = jnp.sin(angles).reshape(bcast_shape)
    vec_f32 = vectors.astype(jnp.float32)
    first_half = vec_f32[..., :half_dim]
    second_half = vec_f32[..., half_dim:]
    rotated = jnp.concatenate([first_half * cos_part - second_half * sin_part, second_half * cos_part + first_half * sin_part], axis=-1)
    return rotated.astype(jnp.bfloat16)


def attend_rows(query_rot, key_rot, value_new, k_cache, v_cache, lengths):
    positions = jnp.arange(k_cache.shape[1], dtype=jnp.int32)
    write_mask = (positions[None, :] == lengths[:, None])[:, :, None]
    k_updated = jnp.where(write_mask, key_rot[:, None, :], k_cache)
    v_updated = jnp.where(write_mask, value_new[:, None, :], v_cache)
    scores = jnp.einsum('rhd,rtd->rht', query_rot, k_updated, preferred_element_type=jnp.float32) * (query_rot.shape[-1] ** -0.5)
    valid_mask = (positions[None, :] <= lengths[:, None])[:, None, :]
    scores = jnp.where(valid_mask, scores, -1e30)
    attn_probs = jax.nn.softmax(scores, axis=-1).astype(jnp.bfloat16)
    attended = jnp.einsum('rht,rtd->rhd', attn_probs, v_updated, preferred_element_type=jnp.float32).astype(jnp.bfloat16)
    return attended, k_updated, v_updated


def cut(w, axis, start, size):
    return lax.dynamic_slice_in_dim(w, start, size, axis=axis)


def dot00(a, b):
    return lax.dot_general(a, b, (((0,), (0,)), ((), ())), preferred_element_type=jnp.float32)


def solution(mesh):
    row_axes = ('dp', 'tx', 'tyz')
    tx_size = mesh.shape['tx']

    def decode_layer(residual, ln_scale, w_query, w_key, w_value, w_gate, w_up, w_out, w_down, k_cache, v_cache, lengths):
        dp, z, ty = lax.axis_index('dp'), lax.axis_index('tx'), lax.axis_index('tyz')
        rows_all, cols = residual.shape
        rows = k_cache.shape[0]
        head_dim = w_key.shape[1]
        model_dim = cols * 16
        k_slice = w_gate.shape[0]
        mlp_half = w_gate.shape[1] // tx_size // 2
        kv_half = 2 * head_dim // 16 // 2
        w_kv = jnp.concatenate([w_key.T, w_value.T], axis=0)
        wq_t = w_query.T

        def qkv_block(target, h):
            return jnp.concatenate([
                cut(wq_t, 0, target * 2 * head_dim + h * head_dim, head_dim),
                cut(w_kv, 0, (target * 4 + ty) * 2 * kv_half + h * kv_half, kv_half)], axis=0)

        def mlp_block(target, h):
            at = (target * 2 + h) * mlp_half
            return jnp.concatenate([cut(w_gate, 1, at, mlp_half), cut(w_up, 1, at, mlp_half)], axis=1)

        def out_block(target, h):
            return jnp.concatenate([
                cut(w_down, 0, (target * 2 + h) * mlp_half, mlp_half),
                cut(w_out, 0, (target * 2 + h) * head_dim, head_dim)], axis=0)

        def exchange(block):
            mine, twin = [block(z, dp)], [block(z, 1 - dp)]
            for o in range(1, NZ):
                got = lax.ppermute(block(lax.rem(z + o, NZ), dp), 'tx', [(i, (i + o) % NZ) for i in range(NZ)])
                mine.append(got)
                twin.append(lax.ppermute(got, 'dp', [(0, 1), (1, 0)]))
            return mine, twin

        scale_rows = jnp.pad(ln_scale[None, :], ((0, EXTRA - 1), (0, rows_all - cols)))
        gathered = gather_blocks(jnp.concatenate([residual.T, scale_rows], axis=0))
        qkv_w = exchange(qkv_block)
        mlp_w = exchange(mlp_block)
        out_w = exchange(out_block)

        res_f32 = gathered[:, :, :cols, :].astype(jnp.float32)
        scale = gathered[:, :, cols, :cols].astype(jnp.float32)
        row_mean = jnp.sum(res_f32, axis=(0, 1, 2)) / model_dim
        row_var = jnp.sum(jnp.square(res_f32 - row_mean), axis=(0, 1, 2)) / model_dim
        normed = ((res_f32 - row_mean) * lax.rsqrt(row_var + LN_EPS) * scale[..., None]).astype(jnp.bfloat16)
        normed = normed.reshape(NZ, 4 * cols, rows_all)

        qkv = []
        for ws in qkv_w:
            acc = sum(jnp.dot(ws[o], normed[o], preferred_element_type=jnp.float32) for o in range(NZ))
            qkv.append(acc.astype(jnp.bfloat16))
        qkv = jnp.concatenate(qkv, axis=0)
        qkv = qkv.reshape(qkv.shape[0], 16, rows).transpose(1, 0, 2)
        qkv = lax.all_to_all(qkv, ('tx', 'tyz'), 0, 0, tiled=True)
        half = head_dim + kv_half
        qkv = qkv.reshape(16, 2, half, rows)
        query = qkv[:, :, :head_dim].reshape(32, head_dim, rows).transpose(2, 0, 1)
        kv = qkv[:, :, head_dim:]
        kv = jnp.where(dp == 0, kv, kv[:, ::-1]).reshape(2 * head_dim, rows).T
        query_rot = rope_rotate(query, lengths)
        key_rot = rope_rotate(kv[:, :head_dim], lengths)
        attended, k_updated, v_updated = attend_rows(query_rot, key_rot, kv[:, head_dim:], k_cache, v_cache, lengths)
        attn = attended.reshape(rows, 16, 2 * head_dim).transpose(1, 0, 2)
        attn = lax.all_to_all(attn, ('tx', 'tyz'), 0, 0, tiled=True).reshape(rows_all, 2, head_dim)

        parts = [0.0] * NZ
        for h, ws in enumerate(mlp_w):
            acc = sum(dot00(normed[o], ws[o]) for o in range(NZ)).astype(jnp.bfloat16)
            gate, up = acc[:, :mlp_half].astype(jnp.float32), acc[:, mlp_half:].astype(jnp.float32)
            act = (jax.nn.silu(gate) * up).astype(jnp.bfloat16)
            lhs = jnp.concatenate([act, attn[:, h]], axis=1)
            for o in range(NZ):
                parts[o] = parts[o] + lax.dot_general(
                    out_w[h][o], lhs, (((0,), (1,)), ((), ())), preferred_element_type=jnp.float32)
        parts = jnp.stack([p.astype(jnp.bfloat16) for p in parts]).reshape(NZ, 4, cols, rows_all)
        new_resid = reduce_blocks(parts, residual.T).T
        return new_resid, k_updated, v_updated

    full = P(row_axes)
    res_spec = P('dp', ('tx', 'tyz'))
    return jax.shard_map(
        decode_layer, mesh=mesh,
        in_specs=(res_spec, P(('tx', 'tyz')), P('tx', 'tyz'), P('tx'), P('tx'), P('tx', 'tyz'), P('tx', 'tyz'),
                  P('tyz', 'tx'), P('tyz', 'tx'), full, full, full),
        out_specs=(res_spec, full, full), check_vma=False)
```

```python
import jax
import jax.numpy as jnp
from jax import lax
from jax.experimental import pallas as pl
from jax.experimental.pallas import tpu as pltpu
from jax.sharding import PartitionSpec as P


LN_EPS = 1e-5
ROPE_BASE = 10000.0
NZ = 4
LANES = 128


def position():
    dp = lax.axis_index("dp")
    z = lax.axis_index("tx")
    ty = lax.axis_index("tyz")
    return dp, z, ty


def others(z, ty):
    for dz in (2, 1, 3, 0):
        for dt in range(4):
            if dz or dt:
                yield dz * 4 + dt - 1, lax.rem(z + dz, NZ), lax.rem(ty + dt, 4)


def source(z, ty, dz, dt):
    return lax.rem(z + NZ - dz, NZ) * 4 + lax.rem(ty + 4 - dt, 4)


def group_barrier(dp, z, ty):
    sem = pltpu.get_barrier_semaphore()
    for _, zt, tt in others(z, ty):
        pl.semaphore_signal(sem, inc=1, device_id=(dp, zt, tt), device_id_type=pl.DeviceIdType.MESH)
    pl.semaphore_signal(sem, inc=1, device_id=(1 - dp, z, ty), device_id_type=pl.DeviceIdType.MESH)
    pl.semaphore_wait(sem, 16)


def remote(src, dst, send_sem, recv_sem, device):
    return pltpu.make_async_remote_copy(src, dst, send_sem, recv_sem, device_id=device,
                                        device_id_type=pl.DeviceIdType.MESH)


def half_rows(dp, size, start=0):
    return pl.ds(pl.multiple_of(dp * size + start, 16), size)


def swap_halves(a, b, low):
    return jnp.where(low, a, pltpu.roll(b, 64, axis=1)), jnp.where(low, pltpu.roll(a, 64, axis=1), b)


def dot00(a, b):
    return lax.dot_general(a, b, (((0,), (0,)), ((), ())), preferred_element_type=jnp.float32)


GATE_EARLY = (1, 3)
LATE = ((0, 2), (1, 2), (1, 1), (1, 3))
TWINNED = 2


def first_kernel(x_ref, wqkv_ref, wg_ref, hn_ref, qkv_ref, gate_ref,
                 gat, wq, q32, packets, lsem, zs, zr, ys, yr, cs, cr,
                 qs, qr, qxs, qxr, gs, gr, gxs, gxr, as_, ar):
    dp, z, ty = position()
    y, c = ty // 2, lax.rem(ty, 2)
    peer_y, peer_c, twin = (1 - y) * 2 + c, y * 2 + 1 - c, (1 - dp, z, ty)
    f32, bf16 = jnp.float32, jnp.bfloat16
    cols, rows = x_ref.shape[0], hn_ref.shape[2]
    width = 4 * cols
    local_x = pltpu.make_async_copy(x_ref, gat.at[0, ty], lsem.at[0])
    local_w = pltpu.make_async_copy(wqkv_ref.at[z], wq.at[:, pl.ds(0, width)], lsem.at[1])
    local_x.start()
    local_w.start()
    group_barrier(dp, z, ty)

    def z_copy(o, step):
        slot = lax.rem(o + step + NZ, NZ)
        return remote(gat.at[o, ty], gat.at[slot, ty], zs.at[o, (step + 1) // 2], zr.at[slot], (dp, z + step, ty))

    def z_arrived(o):
        return remote(gat.at[o, ty], gat.at[o, ty], zs.at[o, 0], zr.at[o], (dp, z, peer_y))

    def y_copy(o, t=ty):
        return remote(gat.at[o, t], gat.at[o, t], ys.at[o], yr.at[o], (dp, z, peer_y))

    def c_copy(o, yy, core=c):
        t = yy * 2 + core
        return remote(gat.at[o, t], gat.at[o, t], cs.at[o, yy], cr.at[o, yy], (dp, z, peer_c))

    head = 80

    def q_copy(o):
        target = lax.rem(z + o, NZ)
        mine = half_rows(dp, head)
        to = (dp, target, ty)
        at = pl.ds(o * width, width)
        return (remote(wqkv_ref.at[target, mine], wq.at[mine, at], qs.at[o, 0], qr.at[o, 0], to),
                remote(wqkv_ref.at[target, pl.ds(2 * head, 16)], wq.at[pl.ds(2 * head, 16), at],
                       qs.at[o, 1], qr.at[o, 1], to))

    def q_pass(o, h):
        part = wq.at[half_rows(h, head), pl.ds(o * width, width)]
        return remote(part, part, qxs.at[o], qxr.at[o], twin)

    half_k = width // 2

    def g_copy(n, o):
        target = lax.rem(z + o, NZ)
        mine = half_rows(dp, half_k)
        return remote(wg_ref.at[mine, pl.ds(pl.multiple_of(target * width, LANES), width)],
                      gate_ref.at[n, mine], gs.at[n], gr.at[n], (dp, target, ty))

    def g_pass(n, h):
        part = gate_ref.at[n, half_rows(h, half_k)]
        return remote(part, part, gxs.at[n], gxr.at[n], twin)

    local_x.wait()
    pl.when(z < NZ - 1)(lambda: z_copy(0, 1).start())
    pl.when(z > 0)(lambda: z_copy(0, -1).start())
    y_copy(0).start()
    c_copy(0, y).start()
    for d in range(1, NZ):
        for o, here, onward, step in (
                (d, z >= d, z < NZ - 1, 1), (NZ - d, z + d < NZ, z > 0, -1)):
            @pl.when(here)
            def _(o=o, onward=onward, step=step):
                z_arrived(o).wait_recv()
                pl.when(onward)(lambda: z_copy(o, step).start())
                y_copy(o).start()
                c_copy(o, y).start()
    for o in (2, 1, 3):
        for copy in q_copy(o):
            copy.start()
    for n, o in enumerate(GATE_EARLY):
        g_copy(n, o).start()
    for d in range(NZ):
        for o, here in ((d, z >= d), (NZ - d, z + d < NZ)):
            if o < NZ:
                @pl.when(here if d else z >= 0)
                def _(o=o):
                    y_copy(o, peer_y).wait_recv()
                    c_copy(o, 1 - y).start()
    for o in (2, 1, 3):
        q_copy(o)[0].wait_recv()
        q_pass(o, dp).start()
    for o in range(NZ):
        for yy in range(2):
            c_copy(o, yy, 1 - c).wait_recv()
    for o in range(NZ):
        y_copy(o).wait_send()
        for yy in range(2):
            c_copy(o, yy).wait_send()

    def fold(v):
        return v.reshape(v.shape[0] // 8, 8, v.shape[1]).sum(axis=0)

    def block(i):
        return gat[i // 4, lax.rem(i, 4), :, pl.ds(0, rows)].astype(f32)

    total = lax.fori_loop(0, 16, lambda i, s: s + fold(block(i)), jnp.zeros((8, rows), f32))
    mean = jnp.sum(total, axis=0, keepdims=True) / (16 * cols)
    total = lax.fori_loop(0, 16, lambda i, s: s + fold(jnp.square(block(i) - mean)), jnp.zeros((8, rows), f32))
    rstd = lax.rsqrt(jnp.sum(total, axis=0, keepdims=True) / (16 * cols) + LN_EPS)

    def normalize(i, carry):
        o, t = i // 4, lax.rem(i, 4)
        scale = gat[o, t, :, pl.ds(rows, LANES)].astype(f32)
        for k in range(rows // LANES):
            at = slice(k * LANES, (k + 1) * LANES)
            v = gat[o, t, :, at].astype(f32)
            hn_ref[o, pl.ds(pl.multiple_of(t * cols, 16), cols), at] = (
                (v - mean[:, at]) * rstd[:, at] * scale).astype(bf16)
        return carry

    lax.fori_loop(0, 16, normalize, 0)

    local_w.wait()
    for o in (2, 1, 3):
        q_copy(o)[1].wait_recv()
        q_pass(o, 1 - dp).wait_recv()
    acc = jnp.dot(wq[:, 0:width], hn_ref[0], preferred_element_type=f32)
    for o in range(1, NZ):
        acc += jnp.dot(wq[:, o * width:(o + 1) * width], hn_ref[o], preferred_element_type=f32)
    q32[...] = acc.astype(bf16).astype(f32)
    low = lax.broadcasted_iota(jnp.int32, (head, LANES), 1) < 64
    for b in range(8):
        at = slice(b * LANES, (b + 1) * LANES)
        even, odd = swap_halves(q32[0:head, at], q32[head:2 * head, at], low)
        kv = q32[2 * head:2 * head + 16, at]
        packets[2 * b] = jnp.concatenate([even, kv], axis=0).astype(bf16)
        packets[2 * b + 1] = jnp.concatenate([odd, kv], axis=0).astype(bf16)
    me = z * 4 + ty

    def a_copy(n, zt, tt):
        return remote(packets.at[zt * 4 + tt], qkv_ref.at[me], as_.at[n], ar.at[n], (dp, zt, tt))

    for n, zt, tt in others(z, ty):
        a_copy(n, zt, tt).start()
    qkv_ref[me] = packets[me]
    for n, o in enumerate(GATE_EARLY):
        g_copy(n, o).wait_recv()
        g_pass(n, dp).start()
    for n, zt, tt in others(z, ty):
        dz, dt = (n + 1) // 4, (n + 1) % 4
        s = source(z, ty, dz, dt)
        remote(packets.at[s], qkv_ref.at[s], as_.at[n], ar.at[n], (dp, zt, tt)).wait_recv()
    for n, o in enumerate(GATE_EARLY):
        g_pass(n, 1 - dp).wait_recv()
        g_pass(n, dp).wait_send()
        g_copy(n, o).wait_send()
    for n, zt, tt in others(z, ty):
        a_copy(n, zt, tt).wait_send()
    for o in range(1, NZ):
        for copy in q_copy(o):
            copy.wait_send()
        q_pass(o, dp).wait_send()
    pl.when(z < NZ - 1)(lambda: z_copy(0, 1).wait_send())
    pl.when(z > 0)(lambda: z_copy(0, -1).wait_send())
    for d in range(1, NZ):
        pl.when(jnp.logical_and(z >= d, z < NZ - 1))(lambda d=d: z_copy(d, 1).wait_send())
        pl.when(jnp.logical_and(z + d < NZ, z > 0))(lambda d=d: z_copy(NZ - d, -1).wait_send())


def first_stage(x_ext, wqkv, w_gate, rows):
    cols = x_ext.shape[0]
    width = 4 * cols
    dma, bf16 = pltpu.SemaphoreType.DMA, jnp.bfloat16
    early = len(GATE_EARLY)
    anywhere, vmem = pl.BlockSpec(memory_space=pl.ANY), pl.BlockSpec(memory_space=pltpu.VMEM)
    return pl.pallas_call(
        first_kernel,
        out_shape=(jax.ShapeDtypeStruct((NZ, width, rows), bf16),
                   jax.ShapeDtypeStruct((16, 96, LANES), bf16),
                   jax.ShapeDtypeStruct((early, width, width), bf16)),
        in_specs=[anywhere] * 3,
        out_specs=(vmem, vmem, anywhere),
        scratch_shapes=[
            pltpu.VMEM((NZ, 4) + x_ext.shape, bf16), pltpu.VMEM((176, NZ * width), bf16),
            pltpu.VMEM((176, rows), jnp.float32), pltpu.VMEM((16, 96, LANES), bf16),
            dma((2,)), dma((NZ, 2)), dma((NZ,)), dma((NZ,)), dma((NZ,)), dma((NZ, 2)), dma((NZ, 2)),
            dma((NZ, 2)), dma((NZ, 2)), dma((NZ,)), dma((NZ,)),
            dma((early,)), dma((early,)), dma((early,)), dma((early,)), dma((15,)), dma((15,))],
        compiler_params=pltpu.CompilerParams(collective_id=0, has_side_effects=True,
                                             vmem_limit_bytes=32 * 2**20),
        name="first_stage",
    )(x_ext, wqkv, w_gate)


def last_kernel(*refs):
    mine_refs, refs = refs[:len(LATE)], refs[len(LATE):]
    twin_refs, refs = refs[:TWINNED], refs[TWINNED:]
    (hn_ref, op_ref, gate_ref, wg_ref, wu_ref, wd_ref, wo_ref, res_ref, out_ref,
                wgu, wdo, wt, lhs, acc, orecv, parts, cbuf, ysend, yrecv, zsend, zrecv,
                lsem, os_, or_, ws, wr, xs, xr, lxs, lxr, cs, cr, ys, yr, zs, zr) = refs
    dp, z, ty = position()
    y, c = ty // 2, lax.rem(ty, 2)
    peer_y, peer_c, twin = (1 - y) * 2 + c, y * 2 + 1 - c, (1 - dp, z, ty)
    f32, bf16 = jnp.float32, jnp.bfloat16
    width = hn_ref.shape[1]
    half_k, head = width // 2, 80
    inner = jnp.logical_and(z > 0, z < NZ - 1)
    early = {o: n for n, o in enumerate(GATE_EARLY)}

    def target_cols(target):
        return pl.ds(pl.multiple_of(target * width, LANES), width)

    local = [pltpu.make_async_copy(wg_ref.at[:, target_cols(z)], wgu.at[0, 0], lsem.at[0]),
             pltpu.make_async_copy(wu_ref.at[:, target_cols(z)], wgu.at[1, 0], lsem.at[1]),
             pltpu.make_async_copy(wd_ref.at[pl.ds(pl.multiple_of(z * width, 16), width)],
                                   wdo.at[0, pl.ds(0, width)], lsem.at[2]),
             pltpu.make_async_copy(wo_ref.at[pl.ds(pl.multiple_of(z * 2 * head, 16), 2 * head)],
                                   wdo.at[0, pl.ds(width, 2 * head)], lsem.at[3])]
    local += [pltpu.make_async_copy(gate_ref.at[n], wgu.at[0, o], lsem.at[4 + n]) for o, n in early.items()]

    def late_half(n, h):
        kind, o = LATE[n]
        return wgu.at[kind, o, half_rows(h, half_k)]

    for n in range(len(LATE)):
        local.append(pltpu.make_async_copy(mine_refs[n], late_half(n, dp), lsem.at[4 + len(early) + n]))
    for n in range(TWINNED):
        local.append(pltpu.make_async_copy(twin_refs[n], late_half(n, 1 - dp),
                                           lsem.at[4 + len(early) + len(LATE) + n]))

    def late_pass(n, h):
        return remote(mine_refs[n], late_half(n, h), lxs.at[n - TWINNED], lxr.at[n - TWINNED], twin)

    for copy in local:
        copy.start()
    group_barrier(dp, z, ty)
    me = z * 4 + ty

    def o_copy(n, zt, tt):
        return remote(op_ref.at[zt * 4 + tt], orecv.at[me], os_.at[n], or_.at[n], (dp, zt, tt))

    for n, zt, tt in others(z, ty):
        o_copy(n, zt, tt).start()
    for n in range(TWINNED, len(LATE)):
        late_pass(n, dp).start()
    orecv[me] = op_ref[me]

    def piece(kind, o, h):
        target = lax.rem(z + o, NZ)
        if kind < 2:
            size = half_k // 2
            start = h * half_k + kind * size
            return (wd_ref.at[pl.ds(pl.multiple_of(target * width + start, 16), size)],
                    wdo.at[o, pl.ds(pl.multiple_of(start, 16), size)])
        return (wo_ref.at[pl.ds(pl.multiple_of((target * 2 + h) * head, 16), head)],
                wdo.at[o, pl.ds(pl.multiple_of(width + h * head, 16), head)])

    def w_copy(kind, o):
        src, dst = piece(kind, o, dp)
        return remote(src, dst, ws.at[kind, o], wr.at[kind, o], (dp, lax.rem(z + o, NZ), ty))

    def w_pass(kind, o, h):
        part = piece(kind, o, h)[1]
        return remote(part, part, xs.at[kind, o], xr.at[kind, o], twin)

    slots = (jnp.where(inner, 2, jnp.where(z == 0, 1, 3)), jnp.where(inner, 1, 2),
             jnp.where(z == NZ - 1, 1, 3))
    out_kinds = (2, 0, 1)
    for s in slots:
        for kind in out_kinds:
            w_copy(kind, lax.rem(NZ - s, NZ)).start()

    def pass_on(kind, o):
        w_copy(kind, o).wait_recv()
        w_pass(kind, o, dp).start()

    def project(kind, o):
        wt[...] = wgu[kind, o].T
        acc[kind] += jnp.dot(wt[...], hn_ref[o], preferred_element_type=f32)

    acc[...] = jnp.zeros_like(acc)
    for copy in local:
        copy.wait()

    def project_step(i, carry):
        project(i // NZ, lax.rem(i, NZ))
        return carry

    lax.fori_loop(0, NZ + 1, project_step, 0)
    for n, (kind, o) in enumerate(LATE[1:], 1):
        if n >= TWINNED:
            late_pass(n, 1 - dp).wait_recv()
        lax.fori_loop(kind * NZ + o, kind * NZ + o + 1, project_step, 0)
    for kind in out_kinds:
        pass_on(kind, slots[0])

    def activate(i, carry):
        at = pl.ds(pl.multiple_of(i * 32, 32), 32)
        gate = acc[0, at].astype(bf16).astype(f32)
        up = acc[1, at].astype(bf16).astype(f32)
        lhs[at] = (jax.nn.silu(gate) * up).astype(bf16)
        return carry

    lax.fori_loop(0, width // 32, activate, 0)

    for n, zt, tt in others(z, ty):
        dz, dt = (n + 1) // 4, (n + 1) % 4
        s = source(z, ty, dz, dt)
        remote(op_ref.at[s], orecv.at[s], os_.at[n], or_.at[n], (dp, zt, tt)).wait_recv()
    low = lax.broadcasted_iota(jnp.int32, (head, LANES), 1) < 64
    for b in range(8):
        at = slice(b * LANES, (b + 1) * LANES)
        first, second = swap_halves(orecv[2 * b].astype(f32), orecv[2 * b + 1].astype(f32), low)
        lhs[width:width + head, at] = first.astype(bf16)
        lhs[width + head:width + 2 * head, at] = second.astype(bf16)

    def c_copy(o, yy):
        return remote(parts.at[o, yy * 2 + 1 - c], cbuf.at[o, yy], cs.at[o, yy], cr.at[o, yy], (dp, z, peer_c))

    def y_copy(o):
        return remote(ysend.at[o], yrecv.at[o], ys.at[o], yr.at[o], (dp, z, peer_y))

    def step_of(o):
        return jnp.where(lax.rem(z - o + NZ, NZ) > z, 1, -1)

    def z_copy(o):
        step = step_of(o)
        slot = lax.rem(o + step + NZ, NZ)
        side = (1 - step) // 2
        return remote(zsend.at[o], zrecv.at[side, slot], zs.at[o], zr.at[side, slot], (dp, z + step, ty))

    def z_arrived(o, side):
        return remote(zsend.at[o], zrecv.at[side, o], zs.at[o], zr.at[side, o], (dp, z, peer_y))

    def multiply(o):
        part = dot00(wdo[o], lhs[...]).astype(bf16)
        for t in range(4):
            parts[o, t] = part[t * (width // 4):(t + 1) * (width // 4)]

    def to_core(o):
        c_copy(o, 1 - y).start()
        c_copy(o, y).start()

    def to_y(o):
        c_copy(o, 1 - y).wait_recv()
        ysend[o] = (parts[o, peer_y].astype(f32) + cbuf[o, 1 - y].astype(f32)).astype(bf16)
        y_copy(o).start()

    def pair_sum(o):
        c_copy(o, y).wait_recv()
        y_copy(o).wait_recv()
        return parts[o, ty].astype(f32) + cbuf[o, y].astype(f32) + yrecv[o].astype(f32)

    def to_z(o):
        total = pair_sum(o)
        side = (1 - step_of(o)) // 2

        @pl.when(inner)
        def _():
            z_arrived(o, side).wait_recv()
            zsend[o] = (total + zrecv[side, o].astype(f32)).astype(bf16)

        @pl.when(jnp.logical_not(inner))
        def _():
            zsend[o] = total.astype(bf16)

        z_copy(o).start()

    def slot_of(k):
        return jnp.where(k == 0, 0, jnp.where(k == 1, slots[0], jnp.where(k == 2, slots[1], slots[2])))

    def output_step(k, carry):
        o = slot_of(k)

        @pl.when(jnp.logical_and(k > 0, k < 3))
        def _():
            for kind in out_kinds:
                pass_on(kind, slot_of(k + 1))

        @pl.when(k > 0)
        def _():
            for kind in out_kinds:
                w_pass(kind, o, 1 - dp).wait_recv()

        multiply(o)
        to_core(o)
        pl.when(k > 0)(lambda: to_y(slot_of(k - 1)))
        pl.when(k > 1)(lambda: to_z(slot_of(k - 1)))
        return carry

    lax.fori_loop(0, NZ, output_step, 0)
    to_y(slots[2])
    to_z(slots[2])

    total = pair_sum(0) + res_ref[...].astype(f32)

    @pl.when(z == 0)
    def _():
        z_arrived(0, 1).wait_recv()
        out_ref[...] = (total + zrecv[1, 0].astype(f32)).astype(bf16)

    @pl.when(z == NZ - 1)
    def _():
        z_arrived(0, 0).wait_recv()
        out_ref[...] = (total + zrecv[0, 0].astype(f32)).astype(bf16)

    @pl.when(inner)
    def _():
        z_arrived(0, 0).wait_recv()
        z_arrived(0, 1).wait_recv()
        out_ref[...] = (total + zrecv[0, 0].astype(f32) + zrecv[1, 0].astype(f32)).astype(bf16)

    for kind, o in [(k, o) for k in out_kinds for o in range(1, NZ)]:
        w_copy(kind, o).wait_send()
        w_pass(kind, o, dp).wait_send()
    for n in range(TWINNED, len(LATE)):
        late_pass(n, dp).wait_send()
    for n, zt, tt in others(z, ty):
        o_copy(n, zt, tt).wait_send()
    for o in range(NZ):
        y_copy(o).wait_send()
        for yy in range(2):
            c_copy(o, yy).wait_send()
        if o:
            z_copy(o).wait_send()


def last_stage(hn, packets, mine, twin, gate, w_gate, w_up, w_down, w_out, residual_t):
    _, width, rows = hn.shape
    cols = width // 4
    dma, bf16 = pltpu.SemaphoreType.DMA, jnp.bfloat16
    anywhere, vmem = pl.BlockSpec(memory_space=pl.ANY), pl.BlockSpec(memory_space=pltpu.VMEM)
    buf = lambda *lead: pltpu.VMEM(lead + (cols, rows), bf16)
    return pl.pallas_call(
        last_kernel,
        out_shape=jax.ShapeDtypeStruct((cols, rows), bf16),
        in_specs=[anywhere] * (len(LATE) + TWINNED) + [vmem, vmem] + [anywhere] * 5 + [vmem], out_specs=vmem,
        scratch_shapes=[
            pltpu.VMEM((2, NZ, width, width), bf16), pltpu.VMEM((NZ, width + 160, width), bf16),
            pltpu.VMEM((width, width), bf16), pltpu.VMEM((width + 160, rows), bf16),
            pltpu.VMEM((2, width, rows), jnp.float32), pltpu.VMEM((16, 80, LANES), bf16),
            buf(NZ, 4), buf(NZ, 2), buf(NZ), buf(NZ), buf(NZ), buf(2, NZ),
            dma((4 + len(GATE_EARLY) + len(LATE) + TWINNED,)), dma((15,)), dma((15,)),
            dma((3, NZ)), dma((3, NZ)), dma((3, NZ)), dma((3, NZ)),
            dma((len(LATE) - TWINNED,)), dma((len(LATE) - TWINNED,)),
            dma((NZ, 2)), dma((NZ, 2)), dma((NZ,)), dma((NZ,)), dma((NZ,)), dma((2, NZ))],
        compiler_params=pltpu.CompilerParams(collective_id=1, has_side_effects=True,
                                             vmem_limit_bytes=56 * 2**20),
        name="last_stage",
    )(*mine, *twin, hn, packets, gate, w_gate, w_up, w_down, w_out, residual_t)


def rope_rotate(vectors, positions):
    head_dim = vectors.shape[-1]
    half_dim = head_dim // 2
    inv_freq = ROPE_BASE ** (-2.0 * jnp.arange(half_dim, dtype=jnp.float32) / head_dim)
    angles = positions.astype(jnp.float32)[:, None] * inv_freq[None, :]
    bcast_shape = (angles.shape[0],) + (1,) * (vectors.ndim - 2) + (half_dim,)
    cos_part = jnp.cos(angles).reshape(bcast_shape)
    sin_part = jnp.sin(angles).reshape(bcast_shape)
    vec_f32 = vectors.astype(jnp.float32)
    first_half = vec_f32[..., :half_dim]
    second_half = vec_f32[..., half_dim:]
    rotated = jnp.concatenate([first_half * cos_part - second_half * sin_part, second_half * cos_part + first_half * sin_part], axis=-1)
    return rotated.astype(jnp.bfloat16)


def attend_rows(query_rot, key_rot, value_new, k_cache, v_cache, lengths):
    positions = jnp.arange(k_cache.shape[1], dtype=jnp.int32)
    write_mask = (positions[None, :] == lengths[:, None])[:, :, None]
    k_updated = jnp.where(write_mask, key_rot[:, None, :], k_cache)
    v_updated = jnp.where(write_mask, value_new[:, None, :], v_cache)
    scores = jnp.einsum('rhd,rtd->rht', query_rot, k_updated, preferred_element_type=jnp.float32) * (query_rot.shape[-1] ** -0.5)
    valid_mask = (positions[None, :] <= lengths[:, None])[:, None, :]
    scores = jnp.where(valid_mask, scores, -1e30)
    attn_probs = jax.nn.softmax(scores, axis=-1).astype(jnp.bfloat16)
    attended = jnp.einsum('rht,rtd->rhd', attn_probs, v_updated, preferred_element_type=jnp.float32).astype(jnp.bfloat16)
    return attended, k_updated, v_updated


def solution(mesh):
    row_axes = ('dp', 'tx', 'tyz')

    def decode_layer(residual, ln_scale, w_query, w_key, w_value, w_gate, w_up, w_out, w_down, k_cache, v_cache, lengths):
        rows_all, cols = residual.shape
        rows = k_cache.shape[0]
        head_dim = w_key.shape[1]
        k_slice = w_gate.shape[0]
        ty = lax.axis_index('tyz')
        wq_t = w_query.T.reshape(NZ, 2 * head_dim, k_slice)
        w_kv = jnp.concatenate([w_key.T, w_value.T], axis=0).reshape(NZ, 4, 10, k_slice)
        w_kv = lax.dynamic_index_in_dim(w_kv, ty, 1, keepdims=False)
        wqkv = jnp.concatenate([wq_t, jnp.pad(w_kv, ((0, 0), (0, 6), (0, 0)))], axis=1)
        x_ext = jnp.concatenate([residual.T, jnp.broadcast_to(ln_scale[:, None], (cols, LANES))], axis=1)
        hn, qkv, gate = first_stage(x_ext, wqkv, w_gate, rows_all)

        dp, z = lax.axis_index('dp'), lax.axis_index('tx')
        half_k, width = k_slice // 2, 4 * cols
        gate_late, up_late, qkv = lax.optimization_barrier((w_gate, w_up, qkv))
        mine, twin = [], []
        for kind, o in LATE:
            block = lax.dynamic_slice((gate_late, up_late)[kind], (dp * half_k, lax.rem(z + o, NZ) * width),
                                      (half_k, width))
            n = len(mine)
            mine.append(lax.ppermute(block, 'tx', [(i, (i + o) % NZ) for i in range(NZ)]))
            if n < TWINNED:
                twin.append(lax.ppermute(mine[-1], 'dp', [(0, 1), (1, 0)]))
        query = qkv[:, :head_dim].reshape(16, head_dim, 2, rows).transpose(3, 0, 2, 1).reshape(rows, 32, head_dim)
        kv = lax.dynamic_slice_in_dim(qkv[:, head_dim:head_dim + 10], lax.rem(ty, 2) * rows, rows, axis=2)
        kv = kv.reshape(2 * head_dim, rows).T
        query_rot = rope_rotate(query, lengths)
        key_rot = rope_rotate(kv[:, :head_dim], lengths)
        attended, k_updated, v_updated = attend_rows(query_rot, key_rot, kv[:, head_dim:], k_cache, v_cache, lengths)
        packets = attended.reshape(rows, 16, 2, head_dim).transpose(1, 3, 2, 0).reshape(16, head_dim, 2 * rows)
        new_resid = last_stage(hn, packets, mine, twin, gate, w_gate, w_up, w_down, w_out, residual.T).T
        return new_resid, k_updated, v_updated

    full = P(row_axes)
    res_spec = P('dp', ('tx', 'tyz'))
    return jax.shard_map(
        decode_layer, mesh=mesh,
        in_specs=(res_spec, P(('tx', 'tyz')), P('tx', 'tyz'), P('tx'), P('tx'), P('tx', 'tyz'), P('tx', 'tyz'),
                  P('tyz', 'tx'), P('tyz', 'tx'), full, full, full),
        out_specs=(res_spec, full, full), check_vma=False)
```

```python
import jax
import jax.numpy as jnp
from jax import lax
from jax.experimental import pallas as pl
from jax.experimental.pallas import tpu as pltpu
from jax.sharding import PartitionSpec as P


LN_EPS = 1e-5
ROPE_BASE = 10000.0
NZ = 4
LANES = 128


def position():
    dp = lax.axis_index("dp")
    z = lax.axis_index("tx")
    ty = lax.axis_index("tyz")
    return dp, z, ty


def others(z, ty):
    for dz in (2, 1, 3, 0):
        for dt in range(4):
            if dz or dt:
                yield dz * 4 + dt - 1, lax.rem(z + dz, NZ), lax.rem(ty + dt, 4)


def source(z, ty, dz, dt):
    return lax.rem(z + NZ - dz, NZ) * 4 + lax.rem(ty + 4 - dt, 4)


def group_barrier(dp, z, ty):
    sem = pltpu.get_barrier_semaphore()
    for _, zt, tt in others(z, ty):
        pl.semaphore_signal(sem, inc=1, device_id=(dp, zt, tt), device_id_type=pl.DeviceIdType.MESH)
    pl.semaphore_signal(sem, inc=1, device_id=(1 - dp, z, ty), device_id_type=pl.DeviceIdType.MESH)
    pl.semaphore_wait(sem, 16)


def remote(src, dst, send_sem, recv_sem, device):
    return pltpu.make_async_remote_copy(src, dst, send_sem, recv_sem, device_id=device,
                                        device_id_type=pl.DeviceIdType.MESH)


def half_rows(dp, size, start=0):
    return pl.ds(pl.multiple_of(dp * size + start, 16), size)


def swap_halves(a, b, low):
    return jnp.where(low, a, pltpu.roll(b, 64, axis=1)), jnp.where(low, pltpu.roll(a, 64, axis=1), b)


def dot00(a, b):
    return lax.dot_general(a, b, (((0,), (0,)), ((), ())), preferred_element_type=jnp.float32)


GATE_EARLY = (1, 3)
LATE = ((0, 2), (1, 2), (1, 1), (1, 3))
TWINNED = 1


def first_kernel(x_ref, scale_ref, wq_ref, wkv_ref, wg_ref, hn_out, qkv_ref, gate_ref,
                 gat, sgat, hn_ref, wqn, wqt, wq, q32, packets, lsem, ss, sr, zs, zr, ys, yr, cs, cr,
                 qs, qr, qxs, qxr, gs, gr, gxs, gxr, as_, ar):
    dp, z, ty = position()
    y, c = ty // 2, lax.rem(ty, 2)
    peer_y, peer_c, twin = (1 - y) * 2 + c, y * 2 + 1 - c, (1 - dp, z, ty)
    f32, bf16 = jnp.float32, jnp.bfloat16
    cols, rows = x_ref.shape
    width = 4 * cols
    local_x = pltpu.make_async_copy(x_ref, gat.at[0, ty], lsem.at[0])
    local_w = pltpu.make_async_copy(wq_ref, wqn, lsem.at[1])
    head = 80

    def kv_rows(target):
        return pl.ds(pl.multiple_of(jnp.minimum(target * 4 + ty, 9) * 16, 16), 16)

    local_kv = pltpu.make_async_copy(wkv_ref.at[kv_rows(z)], wq.at[pl.ds(2 * head, 16), pl.ds(0, width)], lsem.at[2])
    for copy in (local_x, local_w, local_kv):
        copy.start()
    group_barrier(dp, z, ty)

    def z_copy(o, step):
        slot = lax.rem(o + step + NZ, NZ)
        return remote(gat.at[o, ty], gat.at[slot, ty], zs.at[o, (step + 1) // 2], zr.at[slot], (dp, z + step, ty))

    def z_arrived(o):
        return remote(gat.at[o, ty], gat.at[o, ty], zs.at[o, 0], zr.at[o], (dp, z, peer_y))

    def y_copy(o, t=ty):
        return remote(gat.at[o, t], gat.at[o, t], ys.at[o], yr.at[o], (dp, z, peer_y))

    def c_copy(o, yy, core=c):
        t = yy * 2 + core
        return remote(gat.at[o, t], gat.at[o, t], cs.at[o, yy], cr.at[o, yy], (dp, z, peer_c))

    def q_copy(o):
        target = lax.rem(z + o, NZ)
        mine = half_rows(dp, head)
        to = (dp, target, ty)
        at = pl.ds(o * width, width)
        rows_ = pl.ds(pl.multiple_of(target * 2 * head + dp * head, 16), head)
        return (remote(wqt.at[rows_], wq.at[mine, at], qs.at[o, 0], qr.at[o, 0], to),
                remote(wkv_ref.at[kv_rows(target)], wq.at[pl.ds(2 * head, 16), at],
                       qs.at[o, 1], qr.at[o, 1], to))

    def q_pass(o, h):
        part = wq.at[half_rows(h, head), pl.ds(o * width, width)]
        return remote(part, part, qxs.at[o], qxr.at[o], twin)

    half_k = width // 2

    def g_copy(n, o):
        target = lax.rem(z + o, NZ)
        mine = half_rows(dp, half_k)
        return remote(wg_ref.at[mine, pl.ds(pl.multiple_of(target * width, LANES), width)],
                      gate_ref.at[n, mine], gs.at[n], gr.at[n], (dp, target, ty))

    def g_pass(n, h):
        part = gate_ref.at[n, half_rows(h, half_k)]
        return remote(part, part, gxs.at[n], gxr.at[n], twin)

    local_x.wait()
    pl.when(z < NZ - 1)(lambda: z_copy(0, 1).start())
    pl.when(z > 0)(lambda: z_copy(0, -1).start())
    y_copy(0).start()
    c_copy(0, y).start()

    def s_copy(n, zt, tt):
        dz = (n + 1) // 4
        return remote(scale_ref, sgat.at[dz, ty], ss.at[n], sr.at[n], (dp, zt, tt))

    for n, zt, tt in others(z, ty):
        s_copy(n, zt, tt).start()
    local_s = pltpu.make_async_copy(scale_ref, sgat.at[0, ty], lsem.at[3])
    local_s.start()
    local_w.wait()
    wqt[...] = wqn[...].T
    wq[0:2 * head, 0:width] = wqt[pl.ds(pl.multiple_of(z * 2 * head, 16), 2 * head)]
    for d in range(1, NZ):
        for o, here, onward, step in (
                (d, z >= d, z < NZ - 1, 1), (NZ - d, z + d < NZ, z > 0, -1)):
            @pl.when(here)
            def _(o=o, onward=onward, step=step):
                z_arrived(o).wait_recv()
                pl.when(onward)(lambda: z_copy(o, step).start())
                y_copy(o).start()
                c_copy(o, y).start()
    for o in (2, 1, 3):
        for copy in q_copy(o):
            copy.start()
    for n, o in enumerate(GATE_EARLY):
        g_copy(n, o).start()
    for d in range(NZ):
        for o, here in ((d, z >= d), (NZ - d, z + d < NZ)):
            if o < NZ:
                @pl.when(here if d else z >= 0)
                def _(o=o):
                    y_copy(o, peer_y).wait_recv()
                    c_copy(o, 1 - y).start()
    for o in (2, 1, 3):
        q_copy(o)[0].wait_recv()
        q_pass(o, dp).start()
    for o in range(NZ):
        for yy in range(2):
            c_copy(o, yy, 1 - c).wait_recv()
    for o in range(NZ):
        y_copy(o).wait_send()
        for yy in range(2):
            c_copy(o, yy).wait_send()

    def fold(v):
        return v.reshape(v.shape[0] // 8, 8, v.shape[1]).sum(axis=0)

    def block(i):
        return gat[i // 4, lax.rem(i, 4)].astype(f32)

    total = lax.fori_loop(0, 16, lambda i, s: s + fold(block(i)), jnp.zeros((8, rows), f32))
    mean = jnp.sum(total, axis=0, keepdims=True) / (16 * cols)
    total = lax.fori_loop(0, 16, lambda i, s: s + fold(jnp.square(block(i) - mean)), jnp.zeros((8, rows), f32))
    rstd = lax.rsqrt(jnp.sum(total, axis=0, keepdims=True) / (16 * cols) + LN_EPS)

    local_s.wait()
    for n, zt, tt in others(z, ty):
        dz, dt = (n + 1) // 4, (n + 1) % 4
        remote(scale_ref, sgat.at[dz, lax.rem(ty + 4 - dt, 4)], ss.at[n], sr.at[n], (dp, zt, tt)).wait_recv()
    ones = (lax.broadcasted_iota(jnp.int32, (16, LANES), 0) == 0).astype(f32).astype(bf16)

    def normalize(i, carry):
        o, t = i // 4, lax.rem(i, 4)
        scale = dot00(sgat[o, t], ones)[:cols]
        for k in range(rows // LANES):
            at = slice(k * LANES, (k + 1) * LANES)
            v = gat[o, t, :, at].astype(f32)
            hn_ref[o, pl.ds(pl.multiple_of(t * cols, 16), cols), at] = (
                (v - mean[:, at]) * rstd[:, at] * scale).astype(bf16)
        return carry

    lax.fori_loop(0, 16, normalize, 0)
    hn_copy = pltpu.make_async_copy(hn_ref, hn_out, lsem.at[4])
    hn_copy.start()

    local_kv.wait()
    for o in (2, 1, 3):
        q_copy(o)[1].wait_recv()
        q_pass(o, 1 - dp).wait_recv()
    acc = jnp.dot(wq[:, 0:width], hn_ref[0], preferred_element_type=f32)
    for o in range(1, NZ):
        acc += jnp.dot(wq[:, o * width:(o + 1) * width], hn_ref[o], preferred_element_type=f32)
    q32[...] = acc.astype(bf16).astype(f32)
    low = lax.broadcasted_iota(jnp.int32, (head, LANES), 1) < 64
    for b in range(8):
        at = slice(b * LANES, (b + 1) * LANES)
        even, odd = swap_halves(q32[0:head, at], q32[head:2 * head, at], low)
        kv = q32[2 * head:2 * head + 16, at]
        packets[2 * b] = jnp.concatenate([even, kv], axis=0).astype(bf16)
        packets[2 * b + 1] = jnp.concatenate([odd, kv], axis=0).astype(bf16)
    me = z * 4 + ty

    def a_copy(n, zt, tt):
        return remote(packets.at[zt * 4 + tt], qkv_ref.at[me], as_.at[n], ar.at[n], (dp, zt, tt))

    for n, zt, tt in others(z, ty):
        a_copy(n, zt, tt).start()
    qkv_ref[me] = packets[me]
    for n, o in enumerate(GATE_EARLY):
        g_copy(n, o).wait_recv()
        g_pass(n, dp).start()
    for n, zt, tt in others(z, ty):
        dz, dt = (n + 1) // 4, (n + 1) % 4
        s = source(z, ty, dz, dt)
        remote(packets.at[s], qkv_ref.at[s], as_.at[n], ar.at[n], (dp, zt, tt)).wait_recv()
    for n, o in enumerate(GATE_EARLY):
        g_pass(n, 1 - dp).wait_recv()
        g_pass(n, dp).wait_send()
        g_copy(n, o).wait_send()
    hn_copy.wait()
    for n, zt, tt in others(z, ty):
        a_copy(n, zt, tt).wait_send()
        s_copy(n, zt, tt).wait_send()
    for o in range(1, NZ):
        for copy in q_copy(o):
            copy.wait_send()
        q_pass(o, dp).wait_send()
    pl.when(z < NZ - 1)(lambda: z_copy(0, 1).wait_send())
    pl.when(z > 0)(lambda: z_copy(0, -1).wait_send())
    for d in range(1, NZ):
        pl.when(jnp.logical_and(z >= d, z < NZ - 1))(lambda d=d: z_copy(d, 1).wait_send())
        pl.when(jnp.logical_and(z + d < NZ, z > 0))(lambda d=d: z_copy(NZ - d, -1).wait_send())


def first_stage(x, scale, w_query_nat, w_kv, w_gate):
    cols, rows = x.shape
    width = 4 * cols
    dma, bf16 = pltpu.SemaphoreType.DMA, jnp.bfloat16
    early = len(GATE_EARLY)
    anywhere, vmem = pl.BlockSpec(memory_space=pl.ANY), pl.BlockSpec(memory_space=pltpu.VMEM)
    hbm = pl.BlockSpec(memory_space=pltpu.HBM)
    return pl.pallas_call(
        first_kernel,
        out_shape=(jax.ShapeDtypeStruct((NZ, width, rows), bf16),
                   jax.ShapeDtypeStruct((16, 96, LANES), bf16),
                   jax.ShapeDtypeStruct((early, width, width), bf16)),
        in_specs=[hbm] * 5,
        out_specs=(hbm, vmem, hbm),
        scratch_shapes=[
            pltpu.VMEM((NZ, 4, cols, rows), bf16), pltpu.VMEM((NZ, 4, 16, 256), bf16),
            pltpu.VMEM((NZ, width, rows), bf16), pltpu.VMEM((width, width), bf16),
            pltpu.VMEM((width, width), bf16), pltpu.VMEM((176, NZ * width), bf16),
            pltpu.VMEM((176, rows), jnp.float32), pltpu.VMEM((16, 96, LANES), bf16),
            dma((5,)), dma((15,)), dma((15,)), dma((NZ, 2)), dma((NZ,)), dma((NZ,)), dma((NZ,)), dma((NZ, 2)), dma((NZ, 2)),
            dma((NZ, 2)), dma((NZ, 2)), dma((NZ,)), dma((NZ,)),
            dma((early,)), dma((early,)), dma((early,)), dma((early,)), dma((15,)), dma((15,))],
        compiler_params=pltpu.CompilerParams(collective_id=0, has_side_effects=True,
                                             vmem_limit_bytes=60 * 2**20),
        name="first_stage",
    )(x, scale, w_query_nat, w_kv, w_gate)


def last_kernel(*refs):
    mine_refs, refs = refs[:len(LATE)], refs[len(LATE):]
    twin_refs, refs = refs[:TWINNED], refs[TWINNED:]
    (hn_in, op_ref, gate_ref, wg_ref, wu_ref, wd_ref, wo_ref, res_ref, out_ref,
                hn_ref, wgu, wdo, wt, lhs, acc, orecv, parts, cbuf, ysend, yrecv, zsend, zrecv,
                lsem, os_, or_, ws, wr, xs, xr, lxs, lxr, cs, cr, ys, yr, zs, zr) = refs
    dp, z, ty = position()
    y, c = ty // 2, lax.rem(ty, 2)
    peer_y, peer_c, twin = (1 - y) * 2 + c, y * 2 + 1 - c, (1 - dp, z, ty)
    f32, bf16 = jnp.float32, jnp.bfloat16
    width = hn_ref.shape[1]
    half_k, head = width // 2, 80
    inner = jnp.logical_and(z > 0, z < NZ - 1)
    early = {o: n for n, o in enumerate(GATE_EARLY)}

    def target_cols(target):
        return pl.ds(pl.multiple_of(target * width, LANES), width)

    local = [pltpu.make_async_copy(wg_ref.at[:, target_cols(z)], wgu.at[0, 0], lsem.at[0]),
             pltpu.make_async_copy(wu_ref.at[:, target_cols(z)], wgu.at[1, 0], lsem.at[1]),
             pltpu.make_async_copy(wd_ref.at[pl.ds(pl.multiple_of(z * width, 16), width)],
                                   wdo.at[0, pl.ds(0, width)], lsem.at[2]),
             pltpu.make_async_copy(wo_ref.at[pl.ds(pl.multiple_of(z * 2 * head, 16), 2 * head)],
                                   wdo.at[0, pl.ds(width, 2 * head)], lsem.at[3]),
             pltpu.make_async_copy(hn_in, hn_ref, lsem.at[4])]
    local += [pltpu.make_async_copy(gate_ref.at[n], wgu.at[0, o], lsem.at[5 + n]) for o, n in early.items()]

    def late_half(n, h):
        kind, o = LATE[n]
        return wgu.at[kind, o, half_rows(h, half_k)]

    for n in range(len(LATE)):
        local.append(pltpu.make_async_copy(mine_refs[n], late_half(n, dp), lsem.at[5 + len(early) + n]))
    for n in range(TWINNED):
        local.append(pltpu.make_async_copy(twin_refs[n], late_half(n, 1 - dp),
                                           lsem.at[5 + len(early) + len(LATE) + n]))

    def late_pass(n, h):
        return remote(mine_refs[n], late_half(n, h), lxs.at[n - TWINNED], lxr.at[n - TWINNED], twin)

    for copy in local:
        copy.start()
    group_barrier(dp, z, ty)
    me = z * 4 + ty

    def o_copy(n, zt, tt):
        return remote(op_ref.at[zt * 4 + tt], orecv.at[me], os_.at[n], or_.at[n], (dp, zt, tt))

    for n, zt, tt in others(z, ty):
        o_copy(n, zt, tt).start()
    for n in range(TWINNED, len(LATE)):
        late_pass(n, dp).start()
    orecv[me] = op_ref[me]

    def piece(kind, o, h):
        target = lax.rem(z + o, NZ)
        if kind < 2:
            size = half_k // 2
            start = h * half_k + kind * size
            return (wd_ref.at[pl.ds(pl.multiple_of(target * width + start, 16), size)],
                    wdo.at[o, pl.ds(pl.multiple_of(start, 16), size)])
        return (wo_ref.at[pl.ds(pl.multiple_of((target * 2 + h) * head, 16), head)],
                wdo.at[o, pl.ds(pl.multiple_of(width + h * head, 16), head)])

    def w_copy(kind, o):
        src, dst = piece(kind, o, dp)
        return remote(src, dst, ws.at[kind, o], wr.at[kind, o], (dp, lax.rem(z + o, NZ), ty))

    def w_pass(kind, o, h):
        part = piece(kind, o, h)[1]
        return remote(part, part, xs.at[kind, o], xr.at[kind, o], twin)

    slots = (jnp.where(inner, 2, jnp.where(z == 0, 1, 3)), jnp.where(inner, 1, 2),
             jnp.where(z == NZ - 1, 1, 3))
    out_kinds = (2, 0, 1)
    for s in slots:
        for kind in out_kinds:
            w_copy(kind, lax.rem(NZ - s, NZ)).start()

    def pass_on(kind, o):
        w_copy(kind, o).wait_recv()
        w_pass(kind, o, dp).start()

    def project(kind, o):
        wt[...] = wgu[kind, o].T
        acc[kind] += jnp.dot(wt[...], hn_ref[o], preferred_element_type=f32)

    acc[...] = jnp.zeros_like(acc)
    for copy in local:
        copy.wait()

    def project_step(i, carry):
        project(i // NZ, lax.rem(i, NZ))
        return carry

    lax.fori_loop(0, NZ + 1, project_step, 0)
    for n, (kind, o) in enumerate(LATE[1:], 1):
        if n == len(LATE) - 1:
            for k in out_kinds:
                pass_on(k, slots[0])
        if n >= TWINNED:
            late_pass(n, 1 - dp).wait_recv()
        lax.fori_loop(kind * NZ + o, kind * NZ + o + 1, project_step, 0)

    def activate(i, carry):
        at = pl.ds(pl.multiple_of(i * 32, 32), 32)
        gate = acc[0, at].astype(bf16).astype(f32)
        up = acc[1, at].astype(bf16).astype(f32)
        lhs[at] = (jax.nn.silu(gate) * up).astype(bf16)
        return carry

    lax.fori_loop(0, width // 32, activate, 0)

    for n, zt, tt in others(z, ty):
        dz, dt = (n + 1) // 4, (n + 1) % 4
        s = source(z, ty, dz, dt)
        remote(op_ref.at[s], orecv.at[s], os_.at[n], or_.at[n], (dp, zt, tt)).wait_recv()
    low = lax.broadcasted_iota(jnp.int32, (head, LANES), 1) < 64
    for b in range(8):
        at = slice(b * LANES, (b + 1) * LANES)
        first, second = swap_halves(orecv[2 * b].astype(f32), orecv[2 * b + 1].astype(f32), low)
        lhs[width:width + head, at] = first.astype(bf16)
        lhs[width + head:width + 2 * head, at] = second.astype(bf16)

    def c_copy(o, yy):
        return remote(parts.at[o, yy * 2 + 1 - c], cbuf.at[o, yy], cs.at[o, yy], cr.at[o, yy], (dp, z, peer_c))

    def y_copy(o):
        return remote(ysend.at[o], yrecv.at[o], ys.at[o], yr.at[o], (dp, z, peer_y))

    def step_of(o):
        return jnp.where(lax.rem(z - o + NZ, NZ) > z, 1, -1)

    def z_copy(o):
        step = step_of(o)
        slot = lax.rem(o + step + NZ, NZ)
        side = (1 - step) // 2
        return remote(zsend.at[o], zrecv.at[side, slot], zs.at[o], zr.at[side, slot], (dp, z + step, ty))

    def z_arrived(o, side):
        return remote(zsend.at[o], zrecv.at[side, o], zs.at[o], zr.at[side, o], (dp, z, peer_y))

    def multiply(o):
        part = dot00(wdo[o], lhs[...]).astype(bf16)
        for t in range(4):
            parts[o, t] = part[t * (width // 4):(t + 1) * (width // 4)]

    def to_core(o):
        c_copy(o, 1 - y).start()
        c_copy(o, y).start()

    def to_y(o):
        c_copy(o, 1 - y).wait_recv()
        ysend[o] = (parts[o, peer_y].astype(f32) + cbuf[o, 1 - y].astype(f32)).astype(bf16)
        y_copy(o).start()

    def pair_sum(o):
        c_copy(o, y).wait_recv()
        y_copy(o).wait_recv()
        return parts[o, ty].astype(f32) + cbuf[o, y].astype(f32) + yrecv[o].astype(f32)

    def to_z(o):
        total = pair_sum(o)
        side = (1 - step_of(o)) // 2

        @pl.when(inner)
        def _():
            z_arrived(o, side).wait_recv()
            zsend[o] = (total + zrecv[side, o].astype(f32)).astype(bf16)

        @pl.when(jnp.logical_not(inner))
        def _():
            zsend[o] = total.astype(bf16)

        z_copy(o).start()

    def slot_of(k):
        return jnp.where(k == 0, 0, jnp.where(k == 1, slots[0], jnp.where(k == 2, slots[1], slots[2])))

    def output_step(k, carry):
        o = slot_of(k)

        @pl.when(jnp.logical_and(k > 0, k < 3))
        def _():
            for kind in out_kinds:
                pass_on(kind, slot_of(k + 1))

        @pl.when(k > 0)
        def _():
            for kind in out_kinds:
                w_pass(kind, o, 1 - dp).wait_recv()

        multiply(o)
        to_core(o)
        pl.when(k > 0)(lambda: to_y(slot_of(k - 1)))
        pl.when(k > 1)(lambda: to_z(slot_of(k - 1)))
        return carry

    lax.fori_loop(0, NZ, output_step, 0)
    to_y(slots[2])
    to_z(slots[2])

    total = pair_sum(0) + res_ref[...].astype(f32)

    @pl.when(z == 0)
    def _():
        z_arrived(0, 1).wait_recv()
        out_ref[...] = (total + zrecv[1, 0].astype(f32)).astype(bf16)

    @pl.when(z == NZ - 1)
    def _():
        z_arrived(0, 0).wait_recv()
        out_ref[...] = (total + zrecv[0, 0].astype(f32)).astype(bf16)

    @pl.when(inner)
    def _():
        z_arrived(0, 0).wait_recv()
        z_arrived(0, 1).wait_recv()
        out_ref[...] = (total + zrecv[0, 0].astype(f32) + zrecv[1, 0].astype(f32)).astype(bf16)

    for kind, o in [(k, o) for k in out_kinds for o in range(1, NZ)]:
        w_copy(kind, o).wait_send()
        w_pass(kind, o, dp).wait_send()
    for n in range(TWINNED, len(LATE)):
        late_pass(n, dp).wait_send()
    for n, zt, tt in others(z, ty):
        o_copy(n, zt, tt).wait_send()
    for o in range(NZ):
        y_copy(o).wait_send()
        for yy in range(2):
            c_copy(o, yy).wait_send()
        if o:
            z_copy(o).wait_send()


def last_stage(hn, packets, mine, twin, gate, w_gate, w_up, w_down, w_out, residual_t):
    _, width, rows = hn.shape
    cols = width // 4
    dma, bf16 = pltpu.SemaphoreType.DMA, jnp.bfloat16
    anywhere, vmem = pl.BlockSpec(memory_space=pl.ANY), pl.BlockSpec(memory_space=pltpu.VMEM)
    buf = lambda *lead: pltpu.VMEM(lead + (cols, rows), bf16)
    return pl.pallas_call(
        last_kernel,
        out_shape=jax.ShapeDtypeStruct((cols, rows), bf16),
        in_specs=[anywhere] * (len(LATE) + TWINNED) + [pl.BlockSpec(memory_space=pltpu.HBM), vmem] + [anywhere] * 5 + [vmem], out_specs=vmem,
        scratch_shapes=[
            pltpu.VMEM(hn.shape, bf16), pltpu.VMEM((2, NZ, width, width), bf16), pltpu.VMEM((NZ, width + 160, width), bf16),
            pltpu.VMEM((width, width), bf16), pltpu.VMEM((width + 160, rows), bf16),
            pltpu.VMEM((2, width, rows), jnp.float32), pltpu.VMEM((16, 80, LANES), bf16),
            buf(NZ, 4), buf(NZ, 2), buf(NZ), buf(NZ), buf(NZ), buf(2, NZ),
            dma((5 + len(GATE_EARLY) + len(LATE) + TWINNED,)), dma((15,)), dma((15,)),
            dma((3, NZ)), dma((3, NZ)), dma((3, NZ)), dma((3, NZ)),
            dma((len(LATE) - TWINNED,)), dma((len(LATE) - TWINNED,)),
            dma((NZ, 2)), dma((NZ, 2)), dma((NZ,)), dma((NZ,)), dma((NZ,)), dma((2, NZ))],
        compiler_params=pltpu.CompilerParams(collective_id=1, has_side_effects=True,
                                             vmem_limit_bytes=60 * 2**20),
        name="last_stage",
    )(*mine, *twin, hn, packets, gate, w_gate, w_up, w_down, w_out, residual_t)


def rope_rotate(vectors, positions):
    head_dim = vectors.shape[-1]
    half_dim = head_dim // 2
    inv_freq = ROPE_BASE ** (-2.0 * jnp.arange(half_dim, dtype=jnp.float32) / head_dim)
    angles = positions.astype(jnp.float32)[:, None] * inv_freq[None, :]
    bcast_shape = (angles.shape[0],) + (1,) * (vectors.ndim - 2) + (half_dim,)
    cos_part = jnp.cos(angles).reshape(bcast_shape)
    sin_part = jnp.sin(angles).reshape(bcast_shape)
    vec_f32 = vectors.astype(jnp.float32)
    first_half = vec_f32[..., :half_dim]
    second_half = vec_f32[..., half_dim:]
    rotated = jnp.concatenate([first_half * cos_part - second_half * sin_part, second_half * cos_part + first_half * sin_part], axis=-1)
    return rotated.astype(jnp.bfloat16)


def attend_rows(query_rot, key_rot, value_new, k_cache, v_cache, lengths):
    positions = jnp.arange(k_cache.shape[1], dtype=jnp.int32)
    write_mask = (positions[None, :] == lengths[:, None])[:, :, None]
    k_updated = jnp.where(write_mask, key_rot[:, None, :], k_cache)
    v_updated = jnp.where(write_mask, value_new[:, None, :], v_cache)
    scores = jnp.einsum('rhd,rtd->rht', query_rot, k_updated, preferred_element_type=jnp.float32) * (query_rot.shape[-1] ** -0.5)
    valid_mask = (positions[None, :] <= lengths[:, None])[:, None, :]
    scores = jnp.where(valid_mask, scores, -1e30)
    attn_probs = jax.nn.softmax(scores, axis=-1).astype(jnp.bfloat16)
    attended = jnp.einsum('rht,rtd->rhd', attn_probs, v_updated, preferred_element_type=jnp.float32).astype(jnp.bfloat16)
    return attended, k_updated, v_updated


def solution(mesh):
    row_axes = ('dp', 'tx', 'tyz')

    def decode_layer(residual, ln_scale, w_query, w_key, w_value, w_gate, w_up, w_out, w_down, k_cache, v_cache, lengths):
        _, cols = residual.shape
        rows = k_cache.shape[0]
        head_dim = w_key.shape[1]
        k_slice = w_gate.shape[0]
        ty = lax.axis_index('tyz')
        w_kv = jnp.concatenate([w_key.T, w_value.T], axis=0)
        scale = jnp.pad(jnp.broadcast_to(ln_scale[None, :], (16, cols)), ((0, 0), (0, 256 - cols)))
        hn, qkv, gate = first_stage(residual.T, scale, w_query, w_kv, w_gate)

        dp, z = lax.axis_index('dp'), lax.axis_index('tx')
        half_k, width = k_slice // 2, 4 * cols
        gate_late, up_late, qkv = lax.optimization_barrier((w_gate, w_up, qkv))
        mine, twin = [], []
        for kind, o in LATE:
            block = lax.dynamic_slice((gate_late, up_late)[kind], (dp * half_k, lax.rem(z + o, NZ) * width),
                                      (half_k, width))
            n = len(mine)
            mine.append(lax.ppermute(block, 'tx', [(i, (i + o) % NZ) for i in range(NZ)]))
            if n < TWINNED:
                twin.append(lax.ppermute(mine[-1], 'dp', [(0, 1), (1, 0)]))
        query = qkv[:, :head_dim].reshape(16, head_dim, 2, rows).transpose(3, 0, 2, 1).reshape(rows, 32, head_dim)
        kv = lax.dynamic_slice_in_dim(qkv[:10, head_dim:], lax.rem(ty, 2) * rows, rows, axis=2)
        kv = kv.reshape(2 * head_dim, rows).T
        query_rot = rope_rotate(query, lengths)
        key_rot = rope_rotate(kv[:, :head_dim], lengths)
        attended, k_updated, v_updated = attend_rows(query_rot, key_rot, kv[:, head_dim:], k_cache, v_cache, lengths)
        packets = attended.reshape(rows, 16, 2, head_dim).transpose(1, 3, 2, 0).reshape(16, head_dim, 2 * rows)
        new_resid = last_stage(hn, packets, mine, twin, gate, w_gate, w_up, w_down, w_out, residual.T).T
        return new_resid, k_updated, v_updated

    full = P(row_axes)
    res_spec = P('dp', ('tx', 'tyz'))
    return jax.shard_map(
        decode_layer, mesh=mesh,
        in_specs=(res_spec, P(('tx', 'tyz')), P('tx', 'tyz'), P('tx'), P('tx'), P('tx', 'tyz'), P('tx', 'tyz'),
                  P('tyz', 'tx'), P('tyz', 'tx'), full, full, full),
        out_specs=(res_spec, full, full), check_vma=False)
```

```python
import jax
import jax.numpy as jnp
from jax import lax
from jax.experimental import pallas as pl
from jax.experimental.pallas import tpu as pltpu
from jax.sharding import PartitionSpec as P


LN_EPS = 1e-5
ROPE_BASE = 10000.0
NZ = 4
LANES = 128


def position():
    dp = lax.axis_index("dp")
    z = lax.axis_index("tx")
    ty = lax.axis_index("tyz")
    return dp, z, ty


def others(z, ty):
    for dz in (2, 1, 3, 0):
        for dt in range(4):
            if dz or dt:
                yield dz * 4 + dt - 1, lax.rem(z + dz, NZ), lax.rem(ty + dt, 4)


def source(z, ty, dz, dt):
    return lax.rem(z + NZ - dz, NZ) * 4 + lax.rem(ty + 4 - dt, 4)


def group_barrier(dp, z, ty):
    sem = pltpu.get_barrier_semaphore()
    for _, zt, tt in others(z, ty):
        pl.semaphore_signal(sem, inc=1, device_id=(dp, zt, tt), device_id_type=pl.DeviceIdType.MESH)
    pl.semaphore_signal(sem, inc=1, device_id=(1 - dp, z, ty), device_id_type=pl.DeviceIdType.MESH)
    pl.semaphore_wait(sem, 16)


def remote(src, dst, send_sem, recv_sem, device):
    return pltpu.make_async_remote_copy(src, dst, send_sem, recv_sem, device_id=device,
                                        device_id_type=pl.DeviceIdType.MESH)


def half_rows(dp, size, start=0):
    return pl.ds(pl.multiple_of(dp * size + start, 16), size)


def swap_halves(a, b, low):
    return jnp.where(low, a, pltpu.roll(b, 64, axis=1)), jnp.where(low, pltpu.roll(a, 64, axis=1), b)


def dot00(a, b):
    return lax.dot_general(a, b, (((0,), (0,)), ((), ())), preferred_element_type=jnp.float32)


GATE_EARLY = (1, 3)
LATE = ((1, 1), (0, 2), (1, 2), (1, 3))
MOVED = 3
TWINNED = 1


def first_kernel(*refs):
    x_ref, scale_ref, wq_ref, wk_ref, wv_ref, wg_ref, wu_ref, hn_out, qkv_ref, gate_ref = refs[:10]
    late_refs, refs = refs[10:10 + len(LATE)], refs[10 + len(LATE):]
    (sbuf, lbuf, li, lo, ts, tr, gat, sgat, hn_ref, wqn, wqt, wq, q32, packets, lsem, ss, sr, zs, zr, ys, yr, cs, cr,
                 qs, qr, qxs, qxr, gs, gr, gxs, gxr, as_, ar) = refs
    dp, z, ty = position()
    y, c = ty // 2, lax.rem(ty, 2)
    peer_y, peer_c, twin = (1 - y) * 2 + c, y * 2 + 1 - c, (1 - dp, z, ty)
    f32, bf16 = jnp.float32, jnp.bfloat16
    cols, rows = x_ref.shape
    width = 4 * cols
    local_x = pltpu.make_async_copy(x_ref, gat.at[0, ty], lsem.at[0])
    local_w = pltpu.make_async_copy(wq_ref, wqn, lsem.at[1])
    head = 80

    def kv_part(target, act):
        block = jnp.minimum(target * 4 + ty, 9)
        for ref, first in ((wk_ref, 0), (wv_ref, 5)):
            @pl.when(jnp.logical_and(block >= first, block < first + 5))
            def _(ref=ref, first=first):
                act(ref.at[pl.ds(pl.multiple_of((block - first) * 16, 16), 16)])

    def kv_local(src):
        return pltpu.make_async_copy(src, wq.at[pl.ds(2 * head, 16), pl.ds(0, width)], lsem.at[2])

    def late_in(n):
        kind, o = LATE[n]
        cols_ = pl.ds(pl.multiple_of(lax.rem(z + o, NZ) * width, LANES), width)
        return pltpu.make_async_copy((wg_ref, wu_ref)[kind].at[half_rows(dp, width // 2), cols_], lbuf.at[n], li.at[n])

    def late_out(n):
        return pltpu.make_async_copy(lbuf.at[n], late_refs[n], lo.at[n])

    for copy in (local_x, local_w):
        copy.start()
    kv_part(z, lambda src: kv_local(src).start())
    sbuf[...] = jnp.zeros_like(sbuf)
    sbuf[:, 0:cols] = jnp.broadcast_to(scale_ref[...], (16, cols))
    group_barrier(dp, z, ty)

    def z_copy(o, step):
        slot = lax.rem(o + step + NZ, NZ)
        return remote(gat.at[o, ty], gat.at[slot, ty], zs.at[o, (step + 1) // 2], zr.at[slot], (dp, z + step, ty))

    def z_arrived(o):
        return remote(gat.at[o, ty], gat.at[o, ty], zs.at[o, 0], zr.at[o], (dp, z, peer_y))

    def y_copy(o, t=ty):
        return remote(gat.at[o, t], gat.at[o, t], ys.at[o], yr.at[o], (dp, z, peer_y))

    def c_copy(o, yy, core=c):
        t = yy * 2 + core
        return remote(gat.at[o, t], gat.at[o, t], cs.at[o, yy], cr.at[o, yy], (dp, z, peer_c))

    def q_copy(o):
        target = lax.rem(z + o, NZ)
        mine = half_rows(dp, head)
        to = (dp, target, ty)
        at = pl.ds(o * width, width)
        rows_ = pl.ds(pl.multiple_of(target * 2 * head + dp * head, 16), head)
        return remote(wqt.at[rows_], wq.at[mine, at], qs.at[o, 0], qr.at[o, 0], to)

    def kv_copy(o, src):
        return remote(src, wq.at[pl.ds(2 * head, 16), pl.ds(o * width, width)], qs.at[o, 1], qr.at[o, 1],
                      (dp, lax.rem(z + o, NZ), ty))

    def q_pass(o, h):
        part = wq.at[half_rows(h, head), pl.ds(o * width, width)]
        return remote(part, part, qxs.at[o], qxr.at[o], twin)

    half_k = width // 2

    def g_copy(n, o):
        target = lax.rem(z + o, NZ)
        mine = half_rows(dp, half_k)
        return remote(wg_ref.at[mine, pl.ds(pl.multiple_of(target * width, LANES), width)],
                      gate_ref.at[n, mine], gs.at[n], gr.at[n], (dp, target, ty))

    def g_pass(n, h):
        part = gate_ref.at[n, half_rows(h, half_k)]
        return remote(part, part, gxs.at[n], gxr.at[n], twin)

    local_x.wait()
    pl.when(z < NZ - 1)(lambda: z_copy(0, 1).start())
    pl.when(z > 0)(lambda: z_copy(0, -1).start())
    y_copy(0).start()
    c_copy(0, y).start()

    def s_copy(n, zt, tt):
        dz = (n + 1) // 4
        return remote(sbuf, sgat.at[dz, ty], ss.at[n], sr.at[n], (dp, zt, tt))

    for n, zt, tt in others(z, ty):
        s_copy(n, zt, tt).start()
    sgat[0, ty] = sbuf[...]
    for n in range(MOVED):
        late_in(n).start()
    local_w.wait()
    wqt[...] = wqn[...].T
    wq[0:2 * head, 0:width] = wqt[pl.ds(pl.multiple_of(z * 2 * head, 16), 2 * head)]
    for d in range(1, NZ):
        for o, here, onward, step in (
                (d, z >= d, z < NZ - 1, 1), (NZ - d, z + d < NZ, z > 0, -1)):
            @pl.when(here)
            def _(o=o, onward=onward, step=step):
                z_arrived(o).wait_recv()
                pl.when(onward)(lambda: z_copy(o, step).start())
                y_copy(o).start()
                c_copy(o, y).start()
    for o in (2, 1, 3):
        q_copy(o).start()
        kv_part(lax.rem(z + o, NZ), lambda src, o=o: kv_copy(o, src).start())
    for n in range(MOVED):
        late_in(n).wait()
        late_out(n).start()
    for n, o in enumerate(GATE_EARLY):
        g_copy(n, o).start()
    for d in range(NZ):
        for o, here in ((d, z >= d), (NZ - d, z + d < NZ)):
            if o < NZ:
                @pl.when(here if d else z >= 0)
                def _(o=o):
                    y_copy(o, peer_y).wait_recv()
                    c_copy(o, 1 - y).start()
    for o in (2, 1, 3):
        q_copy(o).wait_recv()
        q_pass(o, dp).start()
    for o in range(NZ):
        for yy in range(2):
            c_copy(o, yy, 1 - c).wait_recv()
    for o in range(NZ):
        y_copy(o).wait_send()
        for yy in range(2):
            c_copy(o, yy).wait_send()

    def fold(v):
        return v.reshape(v.shape[0] // 8, 8, v.shape[1]).sum(axis=0)

    def block(i):
        return gat[i // 4, lax.rem(i, 4)].astype(f32)

    total = lax.fori_loop(0, 16, lambda i, s: s + fold(block(i)), jnp.zeros((8, rows), f32))
    mean = jnp.sum(total, axis=0, keepdims=True) / (16 * cols)
    total = lax.fori_loop(0, 16, lambda i, s: s + fold(jnp.square(block(i) - mean)), jnp.zeros((8, rows), f32))
    rstd = lax.rsqrt(jnp.sum(total, axis=0, keepdims=True) / (16 * cols) + LN_EPS)

    for n, zt, tt in others(z, ty):
        dz, dt = (n + 1) // 4, (n + 1) % 4
        remote(sbuf, sgat.at[dz, lax.rem(ty + 4 - dt, 4)], ss.at[n], sr.at[n], (dp, zt, tt)).wait_recv()
    ones = (lax.broadcasted_iota(jnp.int32, (16, LANES), 0) == 0).astype(f32).astype(bf16)

    def normalize(i, carry):
        o, t = i // 4, lax.rem(i, 4)
        scale = dot00(sgat[o, t], ones)[:cols]
        for k in range(rows // LANES):
            at = slice(k * LANES, (k + 1) * LANES)
            v = gat[o, t, :, at].astype(f32)
            hn_ref[o, pl.ds(pl.multiple_of(t * cols, 16), cols), at] = (
                (v - mean[:, at]) * rstd[:, at] * scale).astype(bf16)
        return carry

    lax.fori_loop(0, 16, normalize, 0)
    hn_copy = pltpu.make_async_copy(hn_ref, hn_out, lsem.at[4])
    hn_copy.start()

    kv_local(wk_ref.at[pl.ds(0, 16)]).wait()
    for o in (2, 1, 3):
        kv_copy(o, wk_ref.at[pl.ds(0, 16)]).wait_recv()
        q_pass(o, 1 - dp).wait_recv()
    acc = jnp.dot(wq[:, 0:width], hn_ref[0], preferred_element_type=f32)
    for o in range(1, NZ):
        acc += jnp.dot(wq[:, o * width:(o + 1) * width], hn_ref[o], preferred_element_type=f32)
    q32[...] = acc.astype(bf16).astype(f32)
    low = lax.broadcasted_iota(jnp.int32, (head, LANES), 1) < 64
    for b in range(8):
        at = slice(b * LANES, (b + 1) * LANES)
        even, odd = swap_halves(q32[0:head, at], q32[head:2 * head, at], low)
        kv = q32[2 * head:2 * head + 16, at]
        packets[2 * b] = jnp.concatenate([even, kv], axis=0).astype(bf16)
        packets[2 * b + 1] = jnp.concatenate([odd, kv], axis=0).astype(bf16)
    me = z * 4 + ty

    def a_copy(n, zt, tt):
        return remote(packets.at[zt * 4 + tt], qkv_ref.at[me], as_.at[n], ar.at[n], (dp, zt, tt))

    for n, zt, tt in others(z, ty):
        a_copy(n, zt, tt).start()
    kind, o = LATE[MOVED]
    target = lax.rem(z + o, NZ)
    last_copy = remote((wg_ref, wu_ref)[kind].at[half_rows(dp, half_k),
                                                 pl.ds(pl.multiple_of(target * width, LANES), width)],
                       late_refs[MOVED], ts, tr, (dp, target, ty))
    last_copy.start()
    qkv_ref[me] = packets[me]
    for n, o in enumerate(GATE_EARLY):
        g_copy(n, o).wait_recv()
        g_pass(n, dp).start()
    for n, zt, tt in others(z, ty):
        dz, dt = (n + 1) // 4, (n + 1) % 4
        s = source(z, ty, dz, dt)
        remote(packets.at[s], qkv_ref.at[s], as_.at[n], ar.at[n], (dp, zt, tt)).wait_recv()
    for n, o in enumerate(GATE_EARLY):
        g_pass(n, 1 - dp).wait_recv()
        g_pass(n, dp).wait_send()
        g_copy(n, o).wait_send()
    hn_copy.wait()
    for n in range(MOVED):
        late_out(n).wait()
    last_copy.wait()
    for n, zt, tt in others(z, ty):
        a_copy(n, zt, tt).wait_send()
        s_copy(n, zt, tt).wait_send()
    for o in range(1, NZ):
        q_copy(o).wait_send()
        kv_copy(o, wk_ref.at[pl.ds(0, 16)]).wait_send()
        q_pass(o, dp).wait_send()
    pl.when(z < NZ - 1)(lambda: z_copy(0, 1).wait_send())
    pl.when(z > 0)(lambda: z_copy(0, -1).wait_send())
    for d in range(1, NZ):
        pl.when(jnp.logical_and(z >= d, z < NZ - 1))(lambda d=d: z_copy(d, 1).wait_send())
        pl.when(jnp.logical_and(z + d < NZ, z > 0))(lambda d=d: z_copy(NZ - d, -1).wait_send())


def first_stage(x, scale, w_query_nat, w_k, w_v, w_gate, w_up):
    cols, rows = x.shape
    width = 4 * cols
    dma, bf16 = pltpu.SemaphoreType.DMA, jnp.bfloat16
    early = len(GATE_EARLY)
    anywhere, vmem = pl.BlockSpec(memory_space=pl.ANY), pl.BlockSpec(memory_space=pltpu.VMEM)
    hbm = pl.BlockSpec(memory_space=pltpu.HBM)
    return pl.pallas_call(
        first_kernel,
        out_shape=(jax.ShapeDtypeStruct((NZ, width, rows), bf16),
                   jax.ShapeDtypeStruct((16, 96, LANES), bf16),
                   jax.ShapeDtypeStruct((early, width, width), bf16))
        + (jax.ShapeDtypeStruct((width // 2, width), bf16),) * len(LATE),
        in_specs=[hbm, vmem] + [hbm] * 5,
        out_specs=(hbm, vmem, hbm) + (hbm,) * len(LATE),
        scratch_shapes=[
            pltpu.VMEM((16, 256), bf16), pltpu.VMEM((len(LATE), width // 2, width), bf16),
            dma((len(LATE),)), dma((len(LATE),)), dma, dma,
            pltpu.VMEM((NZ, 4, cols, rows), bf16), pltpu.VMEM((NZ, 4, 16, 256), bf16),
            pltpu.VMEM((NZ, width, rows), bf16), pltpu.VMEM((width, width), bf16),
            pltpu.VMEM((width, width), bf16), pltpu.VMEM((176, NZ * width), bf16),
            pltpu.VMEM((176, rows), jnp.float32), pltpu.VMEM((16, 96, LANES), bf16),
            dma((5,)), dma((15,)), dma((15,)), dma((NZ, 2)), dma((NZ,)), dma((NZ,)), dma((NZ,)), dma((NZ, 2)), dma((NZ, 2)),
            dma((NZ, 2)), dma((NZ, 2)), dma((NZ,)), dma((NZ,)),
            dma((early,)), dma((early,)), dma((early,)), dma((early,)), dma((15,)), dma((15,))],
        compiler_params=pltpu.CompilerParams(collective_id=0, has_side_effects=True,
                                             vmem_limit_bytes=60 * 2**20),
        name="first_stage",
    )(x, scale, w_query_nat, w_k, w_v, w_gate, w_up)


def last_kernel(*refs):
    mine_refs, refs = refs[:len(LATE)], refs[len(LATE):]
    twin_refs, refs = refs[:TWINNED], refs[TWINNED:]
    (hn_in, op_ref, gate_ref, wg_ref, wu_ref, wd_ref, wo_ref, out_ref,
                hn_ref, wgu, wdo, wt, lhs, acc, orecv, parts, cbuf, ysend, yrecv, zsend, zrecv,
                lsem, os_, or_, ws, wr, xs, xr, lxs, lxr, cs, cr, ys, yr, zs, zr) = refs
    dp, z, ty = position()
    y, c = ty // 2, lax.rem(ty, 2)
    peer_y, peer_c, twin = (1 - y) * 2 + c, y * 2 + 1 - c, (1 - dp, z, ty)
    f32, bf16 = jnp.float32, jnp.bfloat16
    width, rows = hn_ref.shape[1], hn_ref.shape[2]
    half_k, head = width // 2, 80
    inner = jnp.logical_and(z > 0, z < NZ - 1)
    early = {o: n for n, o in enumerate(GATE_EARLY)}

    def target_cols(target):
        return pl.ds(pl.multiple_of(target * width, LANES), width)

    local = [pltpu.make_async_copy(wg_ref.at[:, target_cols(z)], wgu.at[0, 0], lsem.at[0]),
             pltpu.make_async_copy(wu_ref.at[:, target_cols(z)], wgu.at[1, 0], lsem.at[1]),
             pltpu.make_async_copy(wd_ref.at[pl.ds(pl.multiple_of(z * width, 16), width)],
                                   wdo.at[0, pl.ds(0, width)], lsem.at[2]),
             pltpu.make_async_copy(wo_ref.at[pl.ds(pl.multiple_of(z * 2 * head, 16), 2 * head)],
                                   wdo.at[0, pl.ds(width, 2 * head)], lsem.at[3]),
             pltpu.make_async_copy(hn_in, hn_ref, lsem.at[4])]
    local += [pltpu.make_async_copy(gate_ref.at[n], wgu.at[0, o], lsem.at[5 + n]) for o, n in early.items()]

    def late_half(n, h):
        kind, o = LATE[n]
        return wgu.at[kind, o, half_rows(h, half_k)]

    for n in range(len(LATE)):
        local.append(pltpu.make_async_copy(mine_refs[n], late_half(n, dp), lsem.at[5 + len(early) + n]))
    for n in range(TWINNED):
        local.append(pltpu.make_async_copy(twin_refs[n], late_half(n, 1 - dp),
                                           lsem.at[5 + len(early) + len(LATE) + n]))

    def late_pass(n, h):
        return remote(mine_refs[n], late_half(n, h), lxs.at[n - TWINNED], lxr.at[n - TWINNED], twin)

    for copy in local:
        copy.start()
    group_barrier(dp, z, ty)
    me = z * 4 + ty

    def o_copy(n, zt, tt):
        return remote(op_ref.at[zt * 4 + tt], orecv.at[me], os_.at[n], or_.at[n], (dp, zt, tt))

    for n, zt, tt in others(z, ty):
        o_copy(n, zt, tt).start()
    for n in range(TWINNED, len(LATE)):
        late_pass(n, dp).start()
    orecv[me] = op_ref[me]

    def piece(kind, o, h):
        target = lax.rem(z + o, NZ)
        if kind < 2:
            size = half_k // 2
            start = h * half_k + kind * size
            return (wd_ref.at[pl.ds(pl.multiple_of(target * width + start, 16), size)],
                    wdo.at[o, pl.ds(pl.multiple_of(start, 16), size)])
        return (wo_ref.at[pl.ds(pl.multiple_of((target * 2 + h) * head, 16), head)],
                wdo.at[o, pl.ds(pl.multiple_of(width + h * head, 16), head)])

    def w_copy(kind, o):
        src, dst = piece(kind, o, dp)
        return remote(src, dst, ws.at[kind, o], wr.at[kind, o], (dp, lax.rem(z + o, NZ), ty))

    def w_pass(kind, o, h):
        part = piece(kind, o, h)[1]
        return remote(part, part, xs.at[kind, o], xr.at[kind, o], twin)

    slots = (jnp.where(inner, 2, jnp.where(z == 0, 1, 3)), jnp.where(inner, 1, 2),
             jnp.where(z == NZ - 1, 1, 3))
    out_kinds = (2, 0, 1)
    for s in slots:
        for kind in out_kinds:
            w_copy(kind, lax.rem(NZ - s, NZ)).start()

    def pass_on(kind, o):
        w_copy(kind, o).wait_recv()
        w_pass(kind, o, dp).start()

    def project(kind, o):
        wt[...] = wgu[kind, o].T
        acc[kind] += jnp.dot(wt[...], hn_ref[o], preferred_element_type=f32)

    acc[...] = jnp.zeros_like(acc)
    for copy in local:
        copy.wait()

    def project_step(i, carry):
        project(i // NZ, lax.rem(i, NZ))
        return carry

    lax.fori_loop(0, 5, lambda i, carry: project_step(jnp.where(i >= 2, i + 1, i), carry), 0)
    for n, (kind, o) in enumerate(LATE[1:], 1):
        if n == len(LATE) - 1:
            for k in out_kinds:
                pass_on(k, slots[0])
        if n >= TWINNED:
            late_pass(n, 1 - dp).wait_recv()
        lax.fori_loop(kind * NZ + o, kind * NZ + o + 1, project_step, 0)

    def activate(i, carry):
        at = pl.ds(pl.multiple_of(i * 32, 32), 32)
        gate = acc[0, at].astype(bf16).astype(f32)
        up = acc[1, at].astype(bf16).astype(f32)
        lhs[at] = (jax.nn.silu(gate) * up).astype(bf16)
        return carry

    lax.fori_loop(0, width // 32, activate, 0)

    for n, zt, tt in others(z, ty):
        dz, dt = (n + 1) // 4, (n + 1) % 4
        s = source(z, ty, dz, dt)
        remote(op_ref.at[s], orecv.at[s], os_.at[n], or_.at[n], (dp, zt, tt)).wait_recv()
    low = lax.broadcasted_iota(jnp.int32, (head, LANES), 1) < 64
    for b in range(8):
        at = slice(b * LANES, (b + 1) * LANES)
        first, second = swap_halves(orecv[2 * b].astype(f32), orecv[2 * b + 1].astype(f32), low)
        lhs[width:width + head, at] = first.astype(bf16)
        lhs[width + head:width + 2 * head, at] = second.astype(bf16)

    def c_copy(o, yy):
        return remote(parts.at[o, yy * 2 + 1 - c], cbuf.at[o, yy], cs.at[o, yy], cr.at[o, yy], (dp, z, peer_c))

    halves = [pl.ds(m * (rows // 2), rows // 2) for m in range(2)]

    def y_copy(o, m):
        return remote(ysend.at[o, :, halves[m]], yrecv.at[o, :, halves[m]], ys.at[o, m], yr.at[o, m], (dp, z, peer_y))

    def step_of(o):
        return jnp.where(lax.rem(z - o + NZ, NZ) > z, 1, -1)

    def z_copy(o, m):
        step = step_of(o)
        slot = lax.rem(o + step + NZ, NZ)
        side = (1 - step) // 2
        return remote(zsend.at[o, :, halves[m]], zrecv.at[side, slot, :, halves[m]],
                      zs.at[o, m], zr.at[side, slot, m], (dp, z + step, ty))

    def z_arrived(o, side, m):
        return remote(zsend.at[o, :, halves[m]], zrecv.at[side, o, :, halves[m]],
                      zs.at[o, m], zr.at[side, o, m], (dp, z, peer_y))

    def multiply(o):
        part = dot00(wdo[o], lhs[...]).astype(bf16)
        for t in range(4):
            parts[o, t] = part[t * (width // 4):(t + 1) * (width // 4)]

    def to_core(o):
        c_copy(o, 1 - y).start()
        c_copy(o, y).start()

    def to_y(o):
        c_copy(o, 1 - y).wait_recv()
        for m, at in enumerate(halves):
            ysend[o, :, at] = (parts[o, peer_y, :, at].astype(f32) + cbuf[o, 1 - y, :, at].astype(f32)).astype(bf16)
            y_copy(o, m).start()

    def pair_sum(o, m):
        at = halves[m]
        y_copy(o, m).wait_recv()
        return parts[o, ty, :, at].astype(f32) + cbuf[o, y, :, at].astype(f32) + yrecv[o, :, at].astype(f32)

    def to_z(o):
        c_copy(o, y).wait_recv()
        side = (1 - step_of(o)) // 2
        for m, at in enumerate(halves):
            total = pair_sum(o, m)

            @pl.when(inner)
            def _():
                z_arrived(o, side, m).wait_recv()
                zsend[o, :, at] = (total + zrecv[side, o, :, at].astype(f32)).astype(bf16)

            @pl.when(jnp.logical_not(inner))
            def _():
                zsend[o, :, at] = total.astype(bf16)

            z_copy(o, m).start()

    def slot_of(k):
        return jnp.where(k == 0, 0, jnp.where(k == 1, slots[0], jnp.where(k == 2, slots[1], slots[2])))

    def output_step(k, carry):
        o = slot_of(k)
        pl.when(k > 0)(lambda: to_y(slot_of(k - 1)))

        @pl.when(jnp.logical_and(k > 0, k < 3))
        def _():
            for kind in out_kinds:
                pass_on(kind, slot_of(k + 1))

        @pl.when(k > 0)
        def _():
            for kind in out_kinds:
                w_pass(kind, o, 1 - dp).wait_recv()

        multiply(o)
        to_core(o)
        pl.when(k > 1)(lambda: to_z(slot_of(k - 1)))
        return carry

    lax.fori_loop(0, NZ, output_step, 0)
    to_y(slots[2])
    to_z(slots[2])

    c_copy(0, y).wait_recv()
    for m, at in enumerate(halves):
        total = pair_sum(0, m)

        @pl.when(z == 0)
        def _():
            z_arrived(0, 1, m).wait_recv()
            out_ref[:, at] = total + zrecv[1, 0, :, at].astype(f32)

        @pl.when(z == NZ - 1)
        def _():
            z_arrived(0, 0, m).wait_recv()
            out_ref[:, at] = total + zrecv[0, 0, :, at].astype(f32)

        @pl.when(inner)
        def _():
            z_arrived(0, 0, m).wait_recv()
            z_arrived(0, 1, m).wait_recv()
            out_ref[:, at] = total + zrecv[0, 0, :, at].astype(f32) + zrecv[1, 0, :, at].astype(f32)

    for kind, o in [(k, o) for k in out_kinds for o in range(1, NZ)]:
        w_copy(kind, o).wait_send()
        w_pass(kind, o, dp).wait_send()
    for n in range(TWINNED, len(LATE)):
        late_pass(n, dp).wait_send()
    for n, zt, tt in others(z, ty):
        o_copy(n, zt, tt).wait_send()
    for o in range(NZ):
        for yy in range(2):
            c_copy(o, yy).wait_send()
        for m in range(2):
            y_copy(o, m).wait_send()
            if o:
                z_copy(o, m).wait_send()


def last_stage(hn, packets, mine, twin, gate, w_gate, w_up, w_down, w_out):
    _, width, rows = hn.shape
    cols = width // 4
    dma, bf16 = pltpu.SemaphoreType.DMA, jnp.bfloat16
    anywhere, vmem = pl.BlockSpec(memory_space=pl.ANY), pl.BlockSpec(memory_space=pltpu.VMEM)
    buf = lambda *lead: pltpu.VMEM(lead + (cols, rows), bf16)
    return pl.pallas_call(
        last_kernel,
        out_shape=jax.ShapeDtypeStruct((cols, rows), jnp.float32),
        in_specs=[anywhere] * (len(LATE) + TWINNED) + [pl.BlockSpec(memory_space=pltpu.HBM), vmem] + [anywhere] * 5, out_specs=vmem,
        scratch_shapes=[
            pltpu.VMEM(hn.shape, bf16), pltpu.VMEM((2, NZ, width, width), bf16), pltpu.VMEM((NZ, width + 160, width), bf16),
            pltpu.VMEM((width, width), bf16), pltpu.VMEM((width + 160, rows), bf16),
            pltpu.VMEM((2, width, rows), jnp.float32), pltpu.VMEM((16, 80, LANES), bf16),
            buf(NZ, 4), buf(NZ, 2), buf(NZ), buf(NZ), buf(NZ), buf(2, NZ),
            dma((5 + len(GATE_EARLY) + len(LATE) + TWINNED,)), dma((15,)), dma((15,)),
            dma((3, NZ)), dma((3, NZ)), dma((3, NZ)), dma((3, NZ)),
            dma((len(LATE) - TWINNED,)), dma((len(LATE) - TWINNED,)),
            dma((NZ, 2)), dma((NZ, 2)), dma((NZ, 2)), dma((NZ, 2)), dma((NZ, 2)), dma((2, NZ, 2))],
        compiler_params=pltpu.CompilerParams(collective_id=1, has_side_effects=True,
                                             vmem_limit_bytes=60 * 2**20),
        name="last_stage",
    )(*mine, *twin, hn, packets, gate, w_gate, w_up, w_down, w_out)


def rope_rotate(vectors, positions):
    head_dim = vectors.shape[-1]
    half_dim = head_dim // 2
    inv_freq = ROPE_BASE ** (-2.0 * jnp.arange(half_dim, dtype=jnp.float32) / head_dim)
    angles = positions.astype(jnp.float32)[:, None] * inv_freq[None, :]
    bcast_shape = (angles.shape[0],) + (1,) * (vectors.ndim - 2) + (half_dim,)
    cos_part = jnp.cos(angles).reshape(bcast_shape)
    sin_part = jnp.sin(angles).reshape(bcast_shape)
    vec_f32 = vectors.astype(jnp.float32)
    first_half = vec_f32[..., :half_dim]
    second_half = vec_f32[..., half_dim:]
    rotated = jnp.concatenate([first_half * cos_part - second_half * sin_part, second_half * cos_part + first_half * sin_part], axis=-1)
    return rotated.astype(jnp.bfloat16)


def attend_rows(query_rot, key_rot, value_new, k_cache, v_cache, lengths):
    positions = jnp.arange(k_cache.shape[1], dtype=jnp.int32)
    write_mask = (positions[None, :] == lengths[:, None])[:, :, None]
    k_updated = jnp.where(write_mask, key_rot[:, None, :], k_cache)
    v_updated = jnp.where(write_mask, value_new[:, None, :], v_cache)
    scores = jnp.einsum('rhd,rtd->rht', query_rot, k_updated, preferred_element_type=jnp.float32) * (query_rot.shape[-1] ** -0.5)
    valid_mask = (positions[None, :] <= lengths[:, None])[:, None, :]
    scores = jnp.where(valid_mask, scores, -1e30)
    attn_probs = jax.nn.softmax(scores, axis=-1).astype(jnp.bfloat16)
    attended = jnp.einsum('rht,rtd->rhd', attn_probs, v_updated, preferred_element_type=jnp.float32).astype(jnp.bfloat16)
    return attended, k_updated, v_updated


def solution(mesh):
    row_axes = ('dp', 'tx', 'tyz')

    def decode_layer(residual, ln_scale, w_query, w_key, w_value, w_gate, w_up, w_out, w_down, k_cache, v_cache, lengths):
        rows = k_cache.shape[0]
        head_dim = w_key.shape[1]
        ty = lax.axis_index('tyz')
        hn, qkv, gate, *late = first_stage(residual.T, ln_scale[None, :], w_query, w_key.T, w_value.T, w_gate, w_up)

        mine, twin = [], []
        for block, (_, o) in zip(late[:MOVED], LATE):
            n = len(mine)
            mine.append(lax.ppermute(block, 'tx', [(i, (i + o) % NZ) for i in range(NZ)]))
            if n < TWINNED:
                twin.append(lax.ppermute(mine[-1], 'dp', [(0, 1), (1, 0)]))
        mine += late[MOVED:]
        query = qkv[:, :head_dim].reshape(16, head_dim, 2, rows).transpose(3, 0, 2, 1).reshape(rows, 32, head_dim)
        kv = lax.dynamic_slice_in_dim(qkv[:10, head_dim:], lax.rem(ty, 2) * rows, rows, axis=2)
        kv = kv.reshape(2 * head_dim, rows).T
        query_rot = rope_rotate(query, lengths)
        key_rot = rope_rotate(kv[:, :head_dim], lengths)
        attended, k_updated, v_updated = attend_rows(query_rot, key_rot, kv[:, head_dim:], k_cache, v_cache, lengths)
        packets = attended.reshape(rows, 16, 2, head_dim).transpose(1, 3, 2, 0).reshape(16, head_dim, 2 * rows)
        block_sum = last_stage(hn, packets, mine, twin, gate, w_gate, w_up, w_down, w_out)
        new_resid = (residual.T.astype(jnp.float32) + block_sum).astype(jnp.bfloat16).T
        return new_resid, k_updated, v_updated

    full = P(row_axes)
    res_spec = P('dp', ('tx', 'tyz'))
    return jax.shard_map(
        decode_layer, mesh=mesh,
        in_specs=(res_spec, P(('tx', 'tyz')), P('tx', 'tyz'), P('tx'), P('tx'), P('tx', 'tyz'), P('tx', 'tyz'),
                  P('tyz', 'tx'), P('tyz', 'tx'), full, full, full),
        out_specs=(res_spec, full, full), check_vma=False)
```
